256 devices in a mesh: row: 8 (over z_hi, y), col: 32 (over z_lo, x, core).
Axes of the slice: x: 4, y: 4, z: 8 (z_hi: 2, z_lo: 4; z = z_hi * 4 + z_lo), core: 2. Of those that a mesh axis runs over, the one named last changes fastest.
Arguments:
- positions: float32 [3, 262144], P(None, ('row', 'col')), may hold values from -6 to 6
- types: int32 [262144], P(('row', 'col')), may hold values from 0 to 4
- radius_type: float32 [5], replicated, may hold values from 0.6 to 1.2
- valence_type: float32 [5], replicated, may hold values from 5 to 60
- bond_depth: float32 [5, 5], replicated, may hold values from 0.02 to 0.2
- pair_tiles: int32 [8, 32, 96, 2], P('row', 'col'), may hold values from 0 to 255, as said below
- tile_count: int32 [8, 32], P('row', 'col'), may hold values from 24 to 96, as said below
Outputs:
- force_energy: float32 [4, 262144], P(None, ('row', 'col'))
The draws below stay inside these ranges and needn't reach their ends.
Inputs may be any that keep to these rules, and one draw needn't show every extreme that they name: `pair_tiles`: each entry is (a, b) with a below 256 and b below 64; the 96 tiles of one device are distinct. Only the first tile_count[r, c] tiles of device (r, c) are live; the most, 96, is reached on some device in every draw.
All inputs are finite; a program needn't handle non-finite values.
Results may differ from the reference program's by a relative error of at most 0.0003.
Values sent between devices are 32-bit elements; how exact they have to be, the bound alone decides.
A program may use at most 64 MiB of HBM per device.

```python
import math
import jax
import jax.numpy as jnp
from jax import lax

ATOM_DEV = 1024
TILES_DEV = 96
TILE = 128
ELEMENTS = 5
ATOMS = 262144
ROW_BLOCKS = 256
COL_BLOCKS = 64
N_ROW = 8
N_COL = 32


def draw_pair_tiles(key, part):
    subkeys = jax.random.split(jax.random.fold_in(key, 11), N_ROW * N_COL)
    chosen = jax.vmap(lambda single: jax.random.permutation(single, ROW_BLOCKS * COL_BLOCKS)[:TILES_DEV])(subkeys)
    chosen = chosen.astype(jnp.int32)
    stacked = jnp.stack([chosen // COL_BLOCKS, chosen % COL_BLOCKS], axis=-1)
    return stacked.reshape(N_ROW, N_COL, TILES_DEV, 2).astype(jnp.int32)


def draw_tile_count(key, part):
    first_key, second_key = jax.random.split(jax.random.fold_in(key, 23))
    counts = jax.random.randint(first_key, (N_ROW * N_COL,), TILES_DEV // 4, TILES_DEV // 2 + 1)
    busiest = jax.random.randint(second_key, (), 0, N_ROW * N_COL)
    spread = counts.at[busiest].set(TILES_DEV)
    return spread.reshape(N_ROW, N_COL).astype(jnp.int32)


def set_ends(drawn, own_key, smallest, high):
    shape = drawn.shape
    place = [jax.random.randint(jax.random.fold_in(own_key, axis), (), 0, shape[axis]) for axis in range(len(shape))]
    drawn = drawn.at[tuple(place)].set(smallest)
    longest = shape.index(max(shape))
    place[longest] = (place[longest] + 1) % shape[longest]
    return drawn.at[tuple(place)].set(high)


def levels(rng, dims, shards, smallest, high):
    def one(position, shards_of):
        draws = jax.random.uniform(jax.random.fold_in(jax.random.fold_in(rng, 6), position), (shards_of,), jnp.float32, smallest / len(shards), high / len(shards))
        return jnp.repeat(jnp.exp(draws), dims[position] // shards_of).reshape((-1,) + (1,) * (len(dims) - position - 1))

    level = one(*shards[0])
    for cut in shards[1:]:
        level = level * one(*cut)
    return level


def gaussian(key, extent, scale, reach, shards=(), held_as=jnp.bfloat16):
    factor_of = levels(key, extent, shards, -0.22, 0.18) if shards else 1.0
    drawn = jax.random.normal(key, extent, jnp.float32) * scale * factor_of
    return jnp.minimum(jnp.maximum(drawn, -reach), reach).astype(held_as)


def setup_inputs(seed: int = 0) -> dict:
    seeds = jax.random.split(jax.random.key(seed), 8)
    positions = gaussian(seeds[0], (3, ATOMS), 1.0, 6.0, ((1, 256),), jnp.float32)
    types = set_ends(jax.random.randint(seeds[1], (ATOMS,), 0, ELEMENTS), jax.random.fold_in(seeds[1], 1), 0, ELEMENTS - 1).astype(jnp.int32)
    radius_type = jnp.clip(jnp.exp(jax.random.uniform(seeds[2], (ELEMENTS,), jnp.float32, math.log(0.6), math.log(1.2))), 0.6, 1.2)
    valence_type = jnp.clip(jnp.exp(jax.random.uniform(seeds[3], (ELEMENTS,), jnp.float32, math.log(5.0), math.log(60.0))), 5.0, 60.0)
    bond_depth = jnp.clip(jnp.exp(jax.random.uniform(seeds[4], (ELEMENTS, ELEMENTS), jnp.float32, math.log(0.02), math.log(0.2))), 0.02, 0.2)
    pair_tiles = draw_pair_tiles(jax.random.fold_in(seeds[7], 71), 0)
    tile_count = draw_tile_count(jax.random.fold_in(seeds[7], 71), 0)
    return {"positions": positions, "types": types, "radius_type": radius_type, "valence_type": valence_type, "bond_depth": bond_depth, "pair_tiles": pair_tiles, "tile_count": tile_count}


def geometry(pos_blocks, radius_blocks, id_blocks, row_idx, col_idx, live_now):
    near_pos = pos_blocks[:, row_idx]
    far_pos = pos_blocks[:, col_idx]
    offset = near_pos[:, :, :, None] - far_pos[:, :, None, :]
    dist_sq = jnp.sum(offset * offset, axis=0)
    rho = 0.5 * (radius_blocks[row_idx][:, :, None] + radius_blocks[col_idx][:, None, :])
    ratio = dist_sq / (rho * rho)
    valid = (id_blocks[row_idx][:, :, None] != id_blocks[col_idx][:, None, :]) & live_now[:, None, None]
    bond_raw = jnp.where(valid, jnp.exp(-(ratio * ratio * ratio)), jnp.float32(0.0))
    return offset, rho, ratio, bond_raw


def reference(positions, types, radius_type, valence_type, bond_depth, pair_tiles, tile_count):
    blocks = ATOMS // TILE
    per_block = ATOM_DEV // TILE
    row_axis = jnp.arange(N_ROW, dtype=jnp.int32)[:, None, None]
    col_axis = jnp.arange(N_COL, dtype=jnp.int32)[None, :, None]
    first = pair_tiles[..., 0]
    second = pair_tiles[..., 1]
    row_global = (row_axis * ROW_BLOCKS + first).astype(jnp.int32)
    col_global = (((second // per_block) * N_COL + col_axis) * per_block + second % per_block).astype(jnp.int32)
    slots = jnp.arange(TILES_DEV, dtype=jnp.int32)[None, None, :]
    live = slots < tile_count[:, :, None]
    row_global = row_global.reshape(-1, 8)
    col_global = col_global.reshape(-1, 8)
    live = live.reshape(-1, 8)
    pos_blocks = positions.reshape(3, blocks, TILE)
    radius_blocks = radius_type[types].reshape(blocks, TILE)
    valence_blocks = valence_type[types].reshape(blocks, TILE)
    type_blocks = types.reshape(blocks, TILE)
    id_blocks = jnp.arange(ATOMS, dtype=jnp.int32).reshape(blocks, TILE)

    def first_pass(total, inputs):
        row_idx, col_idx, live_now = inputs
        offset, rho, ratio, bond_raw = geometry(pos_blocks, radius_blocks, id_blocks, row_idx, col_idx, live_now)
        return total.at[row_idx].add(jnp.sum(bond_raw, axis=2)), None

    coordination, unused = lax.scan(first_pass, jnp.zeros((blocks, TILE), jnp.float32), (row_global, col_global, live))

    def second_pass(total, inputs):
        row_idx, col_idx, live_now = inputs
        offset, rho, ratio, bond_raw = geometry(pos_blocks, radius_blocks, id_blocks, row_idx, col_idx, live_now)
        val_sum = valence_blocks[row_idx][:, :, None] + valence_blocks[col_idx][:, None, :]
        coupling = val_sum / (val_sum + coordination[row_idx][:, :, None] + coordination[col_idx][:, None, :])
        depth_pair = bond_depth[type_blocks[row_idx][:, :, None], type_blocks[col_idx][:, None, :]]
        weight = depth_pair * coupling * bond_raw
        pull = 6.0 * weight * ratio * ratio / (rho * rho)
        forces = -jnp.sum(pull[None] * offset, axis=3)
        energy = -jnp.sum(weight, axis=2)
        terms = jnp.concatenate([forces, energy[None]], axis=0)
        return total.at[:, row_idx].add(terms), None

    result, unused = lax.scan(second_pass, jnp.zeros((4, blocks, TILE), jnp.float32), (row_global, col_global, live))
    return result.reshape(4, ATOMS)
```

```python
import functools

import jax
import jax.numpy as jnp
from jax import lax
from jax.experimental import pallas as pl
from jax.experimental.pallas import tpu as pltpu
from jax.sharding import PartitionSpec as P

TILE = 128
SLOTS = 96
CHIPS = 16
CHUNK = 32
MESH = pl.DeviceIdType.MESH
F32 = jnp.float32


def pieces(value):
    high = value.astype(jnp.bfloat16)
    rest = value - high.astype(F32)
    middle = rest.astype(jnp.bfloat16)
    low = (rest - middle.astype(F32)).astype(jnp.bfloat16)
    return high, middle, low


def by_type(types, table):
    value = jnp.full(types.shape, table[0], F32)
    for t in range(1, len(table)):
        value = jnp.where(types == F32(t), table[t], value)
    return value


def kernel(
    pos_ref, types_ref, radius_ref, valence_ref, depth_ref, tiles_ref, count_ref, out_ref,
    rows, cols, row_radius, row_u, col_u, col_t, col_ub, onehot, parts, store,
    coord_part, coord_in, coord_sum, coord_rx, force_part, force_in, force_sum, force_rx,
    row_send, row_recv, col_send, col_recv, pair_send, pair_recv,
    c_send, c_recv, u_send, u_recv, v_send, v_recv, f_send, f_recv,
):
    r = lax.axis_index("row")
    c = lax.axis_index("col")
    core = lax.rem(c, 2)
    q = c // 2
    z, x = q // 4, lax.rem(q, 4)
    zh, y = r // 4, lax.rem(r, 4)
    other = 1 - core

    def copy(src, dst, send, recv, row, col):
        return pltpu.make_async_remote_copy(
            src_ref=src, dst_ref=dst, send_sem=send, recv_sem=recv,
            device_id=(row, col), device_id_type=MESH,
        )

    chips = [lax.rem(q + k, CHIPS) for k in range(1, CHIPS)]
    rows_of = [lax.rem(r + k, 8) for k in range(1, 8)]

    barrier = pltpu.get_barrier_semaphore()
    for p in chips:
        pl.semaphore_signal(barrier, inc=1, device_id=(r, p * 2 + core), device_id_type=MESH)
    for p in rows_of:
        pl.semaphore_signal(barrier, inc=1, device_id=(p, c), device_id_type=MESH)
    pl.semaphore_signal(barrier, inc=1, device_id=(r, q * 2 + other), device_id_type=MESH)

    own_types = types_ref[...].astype(F32)
    for k in range(8):
        piece = pos_ref[:, k * TILE : (k + 1) * TILE]
        for d in range(3):
            rows[core, q, d, k : k + 1, :] = piece[d : d + 1]
            cols[r, d, k : k + 1, :] = piece[d : d + 1]
    rows[core, q, 3] = own_types
    cols[r, 3] = own_types

    pl.semaphore_wait(barrier, CHIPS - 1 + 7 + 1)

    started = []

    def go(*args):
        descriptor = copy(*args)
        descriptor.start()
        started.append(descriptor)

    def send_row(origin, row, col, slot):
        block = rows.at[core, origin]
        go(block, block, row_send.at[slot], row_recv.at[core, origin], row, col)

    def send_col(origin, row, slot):
        block = cols.at[origin]
        go(block, block, col_send.at[slot], col_recv.at[origin], row, c)

    def device(zz, xx):
        return (zz * 4 + xx) * 2 + core

    far = [lax.rem(z + k, 4) for k in range(1, 4)]
    side = [lax.rem(x + k, 4) for k in range(1, 4)]
    yy = [lax.rem(y + k, 4) for k in range(1, 4)]
    partner = q * 2 + other
    twin = (1 - zh) * 4 + y
    slot = 0
    send_col(r, twin, 0)
    for zz in far:
        send_row(q, r, device(zz, x), slot)
        slot += 1
    for xx in side:
        send_row(q, r, device(z, xx), slot)
        slot += 1
    for k, near in enumerate(yy):
        send_col(r, zh * 4 + near, 1 + k)
    send_row(q, r, partner, slot)
    slot += 1

    def row_wait(par, origin):
        block = rows.at[par, origin]
        copy(block, block, row_send.at[0], row_recv.at[par, origin], r, partner).wait_recv()

    def col_wait(origin):
        block = cols.at[origin]
        copy(block, block, col_send.at[0], col_recv.at[origin], twin, c).wait_recv()

    live = count_ref[0]
    lane = lax.broadcasted_iota(jnp.int32, (8, TILE), 1) // 8
    target = lax.broadcasted_iota(jnp.int32, (256, TILE), 0)
    for m in range(SLOTS // 16):

        def pick(s, held, m=m):
            at = m * 16 + s
            a = tiles_ref[2 * at]
            place = ((a >> 3) & 1) * 128 + (a >> 4) * 8 + (a & 7)
            place = jnp.where(at < live, place, -1)
            return jnp.where(lane == s, place, held)

        held = lax.fori_loop(0, 16, pick, jnp.full((8, TILE), -1, jnp.int32))
        match = target == held[0:1]
        onehot[:, m * TILE : (m + 1) * TILE] = jnp.where(match, F32(1), F32(0)).astype(jnp.bfloat16)

    for zz in far:
        origin = zz * 4 + x
        row_wait(core, origin)
        for xx in side:
            send_row(origin, r, device(z, xx), slot)
            slot += 1
        send_row(origin, r, partner, slot)
        slot += 1
    col_wait(twin)
    for k, near in enumerate(yy):
        send_col(twin, zh * 4 + near, 4 + k)
    for xx in side:
        for k in range(4):
            origin = lax.rem(z + k, 4) * 4 + xx
            row_wait(core, origin)
            send_row(origin, r, partner, slot)
            slot += 1
    for near in yy:
        col_wait(zh * 4 + near)
        col_wait((1 - zh) * 4 + near)

    radius = [radius_ref[t] * F32(0.5) for t in range(5)]
    valence = [valence_ref[t] for t in range(5)]
    for g in range(8):
        kinds = cols[g, 3]
        feats = [cols[g, 0], cols[g, 1], cols[g, 2], by_type(kinds, radius), by_type(kinds, valence)]
        for t in range(5):
            feats.append(by_type(kinds, [depth_ref[5 * t + u] for u in range(5)]))
        while len(feats) < 16:
            feats.append(jnp.zeros((8, TILE), F32))
        turned = jnp.concatenate(feats, axis=0).T
        for k in range(8):
            col_t[g * 8 + k] = turned if k == 0 else pltpu.roll(turned, TILE - k, 1)

    for p in range(CHIPS):
        row_wait(other, p)
    for par in range(2):
        for p in range(CHIPS):
            row_radius[par, p] = by_type(rows[par, p, 3], radius)

    ones_row = lax.broadcasted_iota(jnp.int32, (8, TILE), 0) == 0

    def tile_of(s):
        a = tiles_ref[2 * s]
        b = tiles_ref[2 * s + 1]
        same = (b // 8 == r) & (a // 8 == c) & ((a & 7) == (b & 7))
        return (a >> 3) & 1, a >> 4, a & 7, b, jnp.where(same, F32(1), F32(0))

    def near_row(ref, sp, sq, d, sb):
        return ref[sp, sq, d, pl.ds(sb, 1), :]

    def fold(value):
        return jnp.sum(value.reshape(-1, 8, TILE), axis=0)

    def first(s, carry):
        sp, sq, sb, b, same = tile_of(s)
        near = [near_row(rows, sp, sq, d, sb) for d in range(3)]
        near_r = row_radius[sp, sq, pl.ds(sb, 1), :]
        total = jnp.where(ones_row, -same, F32(0))
        for k in range(TILE // CHUNK):
            far_t = col_t[b, k * CHUNK : (k + 1) * CHUNK, :]
            dist = F32(0)
            for d in range(3):
                offset = near[d] - far_t[:, 8 * d : 8 * d + 1]
                dist = dist + offset * offset
            rho = near_r + far_t[:, 24:25]
            ratio = dist / (rho * rho)
            total = total + fold(jnp.exp(-(ratio * ratio * ratio)))
        parts[0, pl.ds(pl.multiple_of(s * 8, 8), 8), :] = total
        return carry

    lax.fori_loop(0, SLOTS, first, 0)

    def scatter(f):
        total = None
        for piece in pieces(parts[f]):
            term = jnp.dot(onehot[...], piece, preferred_element_type=F32)
            total = term if total is None else total + term
        return total.reshape(2, CHIPS, 8, TILE)

    coord_part[...] = scatter(0)
    go(coord_part.at[other], coord_in, pair_send.at[0], pair_recv.at[0], r, partner)
    mine = coord_part[core]
    copy(coord_part.at[0], coord_in, pair_send.at[0], pair_recv.at[0], r, partner).wait_recv()
    coord_sum[...] = mine + coord_in[...]
    for k, p in enumerate(chips):
        go(coord_sum.at[p], coord_rx.at[q], c_send.at[k], c_recv.at[q], r, p * 2 + core)

    diagonal = [
        jnp.where(
            lax.broadcasted_iota(jnp.int32, (CHUNK, TILE), 0) + k * CHUNK
            == lax.broadcasted_iota(jnp.int32, (CHUNK, TILE), 1),
            F32(1),
            F32(0),
        )
        for k in range(TILE // CHUNK)
    ]

    def prepare(s, carry):
        sp, sq, sb, b, same = tile_of(s)
        near = [near_row(rows, sp, sq, d, sb) for d in range(3)]
        near_r = row_radius[sp, sq, pl.ds(sb, 1), :]
        kinds = near_row(rows, sp, sq, 3, sb)
        near_v = by_type(kinds, valence)
        for k in range(TILE // CHUNK):
            far_t = col_t[b, k * CHUNK : (k + 1) * CHUNK, :]
            offsets = [near[d] - far_t[:, 8 * d : 8 * d + 1] for d in range(3)]
            dist = offsets[0] * offsets[0] + offsets[1] * offsets[1] + offsets[2] * offsets[2]
            rho = near_r + far_t[:, 24:25]
            inverse = F32(1) / (rho * rho)
            ratio = dist * inverse
            square = ratio * ratio
            bond = jnp.exp(-(square * ratio))
            depth = jnp.broadcast_to(far_t[:, 40:41], (CHUNK, TILE))
            for t in range(1, 5):
                depth = jnp.where(kinds == F32(t), far_t[:, 40 + 8 * t : 41 + 8 * t], depth)
            numer = depth * (near_v + far_t[:, 32:33]) * bond
            numer = numer * (F32(1) - same * diagonal[k])
            pull = F32(6) * numer * square * inverse
            at = slice(k * CHUNK, (k + 1) * CHUNK)
            for d in range(3):
                store[s, d, at, :] = pull * offsets[d]
            store[s, 3, at, :] = numer
        return carry

    lax.fori_loop(0, SLOTS // 2, prepare, 0)

    own = coord_sum[q]
    for p in chips:
        copy(coord_sum.at[0], coord_rx.at[p], c_send.at[0], c_recv.at[p], r, p * 2 + core).wait_recv()
        own = own + coord_rx[p]
    own = own + by_type(rows[core, q, 3], valence)
    row_u[core, q] = own
    col_u[r] = own
    for k, p in enumerate(rows_of):
        go(col_u.at[r], col_u.at[r], v_send.at[k], v_recv.at[r], p, c)
    for k, p in enumerate(chips):
        go(row_u.at[core, q], row_u.at[core, q], u_send.at[k], u_recv.at[q], r, p * 2 + core)

    lax.fori_loop(SLOTS // 2, SLOTS, prepare, 0)

    for p in chips:
        block = row_u.at[core, p]
        copy(block, block, u_send.at[0], u_recv.at[p], r, p * 2 + core).wait_recv()
    go(row_u.at[core], row_u.at[core], pair_send.at[1], pair_recv.at[1], r, partner)
    for p in rows_of:
        copy(col_u.at[p], col_u.at[p], v_send.at[0], v_recv.at[p], p, c).wait_recv()
    turned = col_u[...].reshape(64, TILE).T
    for b in range(64):
        col_ub[b] = jnp.broadcast_to(turned[:, b : b + 1], (TILE, TILE))
    copy(row_u.at[other], row_u.at[other], pair_send.at[1], pair_recv.at[1], r, partner).wait_recv()

    def second(s, carry):
        sp, sq, sb, b, unused = tile_of(s)
        near_u = row_u[sp, sq, pl.ds(sb, 1), :]
        total = [jnp.zeros((8, TILE), F32) for d in range(4)]
        for k in range(TILE // CHUNK):
            at = slice(k * CHUNK, (k + 1) * CHUNK)
            scale = F32(1) / (near_u + col_ub[b, at, :])
            for d in range(4):
                total[d] = total[d] - fold(store[s, d, at, :] * scale)
        for d in range(4):
            parts[d, pl.ds(pl.multiple_of(s * 8, 8), 8), :] = total[d]
        return carry

    lax.fori_loop(0, SLOTS, second, 0)

    for d in range(4):
        force_part[:, :, d] = scatter(d)
    go(force_part.at[other], force_in, pair_send.at[2], pair_recv.at[2], r, partner)
    copy(force_part.at[0], force_in, pair_send.at[2], pair_recv.at[2], r, partner).wait_recv()
    force_sum[...] = force_part[core] + force_in[...]
    for k, p in enumerate(chips):
        go(force_sum.at[p], force_rx.at[q], f_send.at[k], f_recv.at[q], r, p * 2 + core)
    own = force_sum[q]
    for p in chips:
        copy(force_sum.at[0], force_rx.at[p], f_send.at[0], f_recv.at[p], r, p * 2 + core).wait_recv()
        own = own + force_rx[p]
    for k in range(8):
        out_ref[:, k * TILE : (k + 1) * TILE] = own[:, k, :]
    for descriptor in started:
        descriptor.wait_send()


def local(positions, types, radius_type, valence_type, bond_depth, pair_tiles, tile_count):
    vmem = pl.BlockSpec(memory_space=pltpu.VMEM)
    smem = pl.BlockSpec(memory_space=pltpu.SMEM)
    dma = pltpu.SemaphoreType.DMA
    return pl.pallas_call(
        kernel,
        out_shape=jax.ShapeDtypeStruct((4, positions.shape[1]), F32),
        in_specs=[vmem, vmem, smem, smem, smem, smem, smem],
        out_specs=vmem,
        scratch_shapes=[
            pltpu.VMEM((2, CHIPS, 4, 8, TILE), F32),
            pltpu.VMEM((8, 4, 8, TILE), F32),
            pltpu.VMEM((2, CHIPS, 8, TILE), F32),
            pltpu.VMEM((2, CHIPS, 8, TILE), F32),
            pltpu.VMEM((8, 8, TILE), F32),
            pltpu.VMEM((64, TILE, TILE), F32),
            pltpu.VMEM((64, TILE, TILE), F32),
            pltpu.VMEM((256, 8 * SLOTS), jnp.bfloat16),
            pltpu.VMEM((4, 8 * SLOTS, TILE), F32),
            pltpu.VMEM((SLOTS, 4, TILE, TILE), F32),
            pltpu.VMEM((2, CHIPS, 8, TILE), F32),
            pltpu.VMEM((CHIPS, 8, TILE), F32),
            pltpu.VMEM((CHIPS, 8, TILE), F32),
            pltpu.VMEM((CHIPS, 8, TILE), F32),
            pltpu.VMEM((2, CHIPS, 4, 8, TILE), F32),
            pltpu.VMEM((CHIPS, 4, 8, TILE), F32),
            pltpu.VMEM((CHIPS, 4, 8, TILE), F32),
            pltpu.VMEM((CHIPS, 4, 8, TILE), F32),
            dma((31,)), dma((2, CHIPS)), dma((7,)), dma((8,)), dma((3,)), dma((3,)),
            dma((15,)), dma((CHIPS,)), dma((15,)), dma((CHIPS,)), dma((7,)), dma((8,)),
            dma((15,)), dma((CHIPS,)),
        ],
        compiler_params=pltpu.CompilerParams(
            collective_id=0, has_side_effects=True, vmem_limit_bytes=60 * 1024 * 1024
        ),
    )(
        positions,
        types.reshape(8, TILE),
        radius_type,
        valence_type,
        bond_depth.reshape(-1),
        pair_tiles.reshape(-1),
        tile_count.reshape(-1),
    )


def solution(mesh):
    in_specs = (
        P(None, ("row", "col")),
        P(("row", "col")),
        P(),
        P(),
        P(),
        P("row", "col", None, None),
        P("row", "col"),
    )
    out_specs = P(None, ("row", "col"))
    return jax.shard_map(local, mesh=mesh, in_specs=in_specs, out_specs=out_specs, check_vma=False)
```

```python
import functools

import jax
import jax.numpy as jnp
from jax import lax
from jax.experimental import pallas as pl
from jax.experimental.pallas import tpu as pltpu
from jax.sharding import PartitionSpec as P

TILE = 128
SLOTS = 96
EARLY = 36
CHIPS = 16
MESH = pl.DeviceIdType.MESH
F32 = jnp.float32
BF16 = jnp.bfloat16
LOG2E = 1.4426950408889634


def pieces(value):
    high = value.astype(BF16).astype(F32)
    rest = value - high
    middle = rest.astype(BF16).astype(F32)
    return high, middle, rest - middle


def by_type(types, table):
    value = jnp.full(types.shape, table[0], F32)
    for t in range(1, len(table)):
        value = jnp.where(types == F32(t), table[t], value)
    return value


def kernel(
    pos_ref, types_ref, radius_ref, valence_ref, depth_ref, tiles_ref, count_ref, out_ref,
    rows, cols, row_radius, row_u, col_u, pick_ref, wide, wide_u, col_w, buf_a, buf_b, onehot, parts, store,
    coord_part, coord_in, coord_sum, coord_rx, force_part, force_in, force_sum, force_rx,
    row_send, row_recv, col_send, col_recv, pair_send, pair_recv,
    c_send, c_recv, u_send, u_recv, v_send, v_recv, f_send, f_recv,
):
    r = lax.axis_index("row")
    c = lax.axis_index("col")
    core = lax.rem(c, 2)
    q = c // 2
    z, x = q // 4, lax.rem(q, 4)
    zh, y = r // 4, lax.rem(r, 4)
    other = 1 - core

    def copy(src, dst, send, recv, row, col):
        return pltpu.make_async_remote_copy(
            src_ref=src, dst_ref=dst, send_sem=send, recv_sem=recv,
            device_id=(row, col), device_id_type=MESH,
        )

    chips = [lax.rem(q + k, CHIPS) for k in range(1, CHIPS)]
    rows_of = [lax.rem(r + k, 8) for k in range(1, 8)]

    def device(zz, xx):
        return (zz * 4 + xx) * 2 + core

    far = [lax.rem(z + k, 4) for k in range(1, 4)]
    side = [lax.rem(x + k, 4) for k in range(1, 4)]
    yy = [lax.rem(y + k, 4) for k in range(1, 4)]
    partner = q * 2 + other
    twin = (1 - zh) * 4 + y
    greeted = [(twin, c)]
    greeted += [(r, device(zz, x)) for zz in far]
    greeted += [(r, device(z, xx)) for xx in side]
    greeted += [(zh * 4 + near, c) for near in yy]
    greeted += [(r, partner)]
    barrier = pltpu.get_barrier_semaphore()
    for row, col in greeted:
        pl.semaphore_signal(barrier, inc=1, device_id=(row, col), device_id_type=MESH)

    own_types = types_ref[...].astype(F32)
    for k in range(8):
        piece = pos_ref[:, k * TILE : (k + 1) * TILE]
        for d in range(3):
            rows[core, q, d, k : k + 1, :] = piece[d : d + 1]
            cols[r, d, k : k + 1, :] = piece[d : d + 1]
    rows[core, q, 3] = own_types
    cols[r, 3] = own_types

    sub = lax.broadcasted_iota(jnp.int32, (8, TILE), 0)
    blank = jnp.zeros((8, TILE), F32)
    for k in range(8):
        mark = jnp.where(sub == k, F32(1), F32(0))
        for d in range(4):
            column = [mark if 3 * d <= f < 3 * d + 3 else blank for f in range(16)]
            m = d * 8 + k
            at = slice(m % 2 * TILE, m % 2 * TILE + TILE)
            pick_ref[m // 2, :, at] = jnp.concatenate(column, axis=0).astype(BF16)

    pl.semaphore_wait(barrier, len(greeted))

    started = []

    def go(*args):
        descriptor = copy(*args)
        descriptor.start()
        started.append(descriptor)

    def send_row(origin, row, col, slot):
        block = rows.at[core, origin]
        go(block, block, row_send.at[slot], row_recv.at[core, origin], row, col)

    def send_col(origin, row, slot):
        block = cols.at[origin]
        go(block, block, col_send.at[slot], col_recv.at[origin], row, c)

    slot = 0
    send_col(r, twin, 0)
    for zz in far:
        send_row(q, r, device(zz, x), slot)
        slot += 1
    for xx in side:
        send_row(q, r, device(z, xx), slot)
        slot += 1
    for k, near in enumerate(yy):
        send_col(r, zh * 4 + near, 1 + k)
    send_row(q, r, partner, slot)
    slot += 1

    def row_wait(par, origin):
        block = rows.at[par, origin]
        copy(block, block, row_send.at[0], row_recv.at[par, origin], r, partner).wait_recv()

    def col_wait(origin):
        block = cols.at[origin]
        copy(block, block, col_send.at[0], col_recv.at[origin], twin, c).wait_recv()

    live = count_ref[0, 0]
    lane = lax.broadcasted_iota(jnp.int32, (8, TILE), 1) // 8
    target = lax.broadcasted_iota(jnp.int32, (256, TILE), 0)
    for m in range(SLOTS // 16):

        def pick(s, held, m=m):
            at = m * 16 + s
            a = tiles_ref[0, at]
            place = ((a >> 3) & 1) * 128 + (a >> 4) * 8 + (a & 7)
            place = jnp.where(at < live, place, -1)
            return jnp.where(lane == s, place, held)

        held = lax.fori_loop(0, 16, pick, jnp.full((8, TILE), -1, jnp.int32))
        match = target == held[0:1]
        onehot[:, m * TILE : (m + 1) * TILE] = jnp.where(match, F32(1), F32(0)).astype(BF16)

    radius = [radius_ref[t] * F32(0.5) for t in range(5)]
    valence = [valence_ref[t] for t in range(5)]

    def turn(feats):
        feats = feats + [blank] * (16 - len(feats))
        return jnp.concatenate(feats, axis=0).T.astype(BF16)

    def lanes_of(left, put_block):
        for m in range(16):
            pair = jnp.dot(left, pick_ref[m], preferred_element_type=F32)
            for h in range(2):
                put_block((2 * m + h) // 8, (2 * m + h) % 8, pair[:, h * TILE : (h + 1) * TILE].reshape(16, 8, TILE))

    def widen(g):
        feats = []
        for value in (cols[g, 0], cols[g, 1], cols[g, 2], by_type(cols[g, 3], radius)):
            feats.extend(pieces(value))

        def put_block(d, k, value):
            wide[g * 8 + k, :, d] = value

        lanes_of(turn(feats), put_block)

    for zz in far:
        origin = zz * 4 + x
        row_wait(core, origin)
        for xx in side:
            send_row(origin, r, device(z, xx), slot)
            slot += 1
        send_row(origin, r, partner, slot)
        slot += 1
    widen(r)
    col_wait(twin)
    for k, near in enumerate(yy):
        send_col(twin, zh * 4 + near, 4 + k)

    def relay(k):
        for xx in side:
            origin = lax.rem(z + k, 4) * 4 + xx
            row_wait(core, origin)
            send_row(origin, r, partner, slots.pop())

    slots = list(range(slot, slot + 12))
    relay(0)

    def near_cols(k, carry):
        origin = zh * 4 + lax.rem(y + k, 4)
        col_wait(origin)
        widen(origin)
        return carry

    lax.fori_loop(1, 4, near_cols, 0)
    for k in range(1, 4):
        relay(k)
    widen(twin)

    def far_cols(k, carry):
        origin = (1 - zh) * 4 + lax.rem(y + k, 4)
        col_wait(origin)
        widen(origin)
        return carry

    lax.fori_loop(1, 4, far_cols, 0)
    for p in range(CHIPS):
        row_wait(other, p)
    for par in range(2):
        for p in range(CHIPS):
            row_radius[par, p] = by_type(rows[par, p, 3], radius)

    def tile_of(s):
        a = tiles_ref[0, s]
        b = tiles_ref[1, s]
        return (a >> 3) & 1, a >> 4, a & 7, b

    def same_block(s):
        a = tiles_ref[0, s]
        b = tiles_ref[1, s]
        same = ((b >> 3) == r) & ((a >> 3) == c) & ((a & 7) == (b & 7))
        return jnp.where(same, F32(1), F32(0))

    def near_rows(s):
        sp, sq, sb, b = tile_of(s)
        near = [rows[sp, sq, d, pl.ds(sb, 1), :] for d in range(3)]
        return near, row_radius[sp, sq, pl.ds(sb, 1), :], b

    def over_tiles(fill, use, begin, end):
        fill(begin, buf_a)

        def body(t, carry):
            s = begin + 2 * t
            fill(s + 1, buf_b)
            use(s, buf_a)
            fill(jnp.minimum(s + 2, SLOTS - 1), buf_a)
            use(s + 1, buf_b)
            return carry

        lax.fori_loop(0, (end - begin) // 2, body, 0)

    def put(d, s, value):
        parts[d, pl.ds(pl.multiple_of(s * 8, 8), 8), :] = value

    def first(s, carry):
        near, near_r, b = near_rows(s)
        total = jnp.where(sub == 0, -same_block(s), F32(0))
        for k in range(16):
            dist = F32(0)
            for d in range(3):
                offset = near[d] - wide[b, k, d]
                dist = dist + offset * offset
            rho = near_r + wide[b, k, 3]
            ratio = dist / (rho * rho)
            total = total + jnp.exp2((ratio * ratio) * (ratio * F32(-LOG2E)))
        put(0, s, total)
        return carry

    lax.fori_loop(0, SLOTS, first, 0)

    def scatter(value):
        high = value.astype(BF16)
        low = (value - high.astype(F32)).astype(BF16)
        return high, low

    def spots(value):
        return value.reshape(2, CHIPS, 8, TILE)

    both = jnp.concatenate(scatter(parts[0]), axis=1)
    both = jnp.dot(onehot[...], both, preferred_element_type=F32)
    coord_part[...] = spots(both[:, :TILE] + both[:, TILE:])
    go(coord_part.at[other], coord_in, pair_send.at[0], pair_recv.at[0], r, partner)
    mine = coord_part[core]
    copy(coord_part.at[0], coord_in, pair_send.at[0], pair_recv.at[0], r, partner).wait_recv()
    coord_sum[...] = mine + coord_in[...]
    for k, p in enumerate(chips):
        go(coord_sum.at[p], coord_rx.at[q], c_send.at[k], c_recv.at[q], r, p * 2 + core)

    lane_at = lax.broadcasted_iota(jnp.int32, (8, TILE), 1)
    for g in range(8):
        feats = []
        for t in range(5):
            table = [depth_ref[t, u] * (valence[t] + valence[u]) for u in range(5)]
            feats.extend(pieces(by_type(cols[g, 3], table)))
        col_w[g] = turn(feats)

    def pair_terms(s, buf):
        sp, sq, sb, b = tile_of(s)
        kinds = jnp.broadcast_to(rows[sp, sq, 3, pl.ds(sb, 1), :], (8, TILE))
        kinds = jnp.where(sub == (b & 7), kinds, F32(-1))
        right = []
        for t in range(5):
            right.extend([jnp.where(kinds == F32(t), F32(1), F32(0))] * 3)
        right = jnp.concatenate(right + [blank], axis=0).astype(BF16)
        buf[...] = jnp.dot(col_w[b >> 3], right, preferred_element_type=F32)

    def prepare(s, buf):
        near, near_r, b = near_rows(s)
        same = same_block(s)
        for k in range(16):
            dx, dy, dz = (near[d] - wide[b, k, d] for d in range(3))
            rho = near_r + wide[b, k, 3]
            inverse = F32(1) / (rho * rho)
            ratio = (dx * dx + dy * dy + dz * dz) * inverse
            square = ratio * ratio
            numer = buf[8 * k : 8 * k + 8, :] * jnp.exp2(square * (ratio * F32(-LOG2E)))
            numer = jnp.where(lane_at == sub + 8 * k, numer * (F32(1) - same), numer)
            pull = numer * (square * inverse)
            store[s, k, 0] = pull * dx
            store[s, k, 1] = pull * dy
            store[s, k, 2] = pull * dz
            store[s, k, 3] = numer

    over_tiles(pair_terms, prepare, 0, EARLY)

    own = coord_sum[q]
    for p in chips:
        copy(coord_sum.at[0], coord_rx.at[p], c_send.at[0], c_recv.at[p], r, p * 2 + core).wait_recv()
        own = own + coord_rx[p]
    own = own + by_type(rows[core, q, 3], valence)
    row_u[core, q] = own
    col_u[r] = own
    for k, p in enumerate(rows_of):
        go(col_u.at[r], col_u.at[r], v_send.at[k], v_recv.at[r], p, c)
    for k, p in enumerate(chips):
        go(row_u.at[core, q], row_u.at[core, q], u_send.at[k], u_recv.at[q], r, p * 2 + core)

    over_tiles(pair_terms, prepare, EARLY, SLOTS)

    for p in chips:
        block = row_u.at[core, p]
        copy(block, block, u_send.at[0], u_recv.at[p], r, p * 2 + core).wait_recv()
    go(row_u.at[core], row_u.at[core], pair_send.at[1], pair_recv.at[1], r, partner)
    for p in rows_of:
        copy(col_u.at[p], col_u.at[p], v_send.at[0], v_recv.at[p], p, c).wait_recv()
    for g in range(2):
        feats = []
        for k in range(4):
            feats.extend(pieces(col_u[4 * g + k]))

        def put_u(d, k, value, g=g):
            wide_u[g * 32 + d * 8 + k] = value

        lanes_of(turn(feats), put_u)
    copy(row_u.at[other], row_u.at[other], pair_send.at[1], pair_recv.at[1], r, partner).wait_recv()

    def second(s, carry):
        sp, sq, sb, b = tile_of(s)
        near = row_u[sp, sq, pl.ds(sb, 1), :]
        total = [F32(0)] * 4
        for k in range(16):
            scale = F32(1) / (near + wide_u[b, k])
            for d in range(4):
                total[d] = total[d] + store[s, k, d] * scale
        for d in range(4):
            put(d, s, total[d])
        return carry

    lax.fori_loop(0, SLOTS, second, 0)

    for d in (0, 2):
        high, low = scatter(jnp.concatenate([parts[d], parts[d + 1]], axis=1))
        both = jnp.dot(onehot[...], high, preferred_element_type=F32)
        both = both + jnp.dot(onehot[...], low, preferred_element_type=F32)
        force_part[:, :, d] = spots(both[:, :TILE])
        force_part[:, :, d + 1] = spots(both[:, TILE:])
    go(force_part.at[other], force_in, pair_send.at[2], pair_recv.at[2], r, partner)
    copy(force_part.at[0], force_in, pair_send.at[2], pair_recv.at[2], r, partner).wait_recv()
    force_sum[...] = force_part[core] + force_in[...]
    for k, p in enumerate(chips):
        go(force_sum.at[p], force_rx.at[q], f_send.at[k], f_recv.at[q], r, p * 2 + core)
    own = force_sum[q]
    for p in chips:
        copy(force_sum.at[0], force_rx.at[p], f_send.at[0], f_recv.at[p], r, p * 2 + core).wait_recv()
        own = own + force_rx[p]
    for k in range(8):
        out_ref[:, k * TILE : (k + 1) * TILE] = own[:, k, :]
    for descriptor in started:
        descriptor.wait_send()


def local(positions, types, radius_type, valence_type, bond_depth, pair_tiles, tile_count):
    vmem = pl.BlockSpec(memory_space=pltpu.VMEM)
    smem = pl.BlockSpec(memory_space=pltpu.SMEM)
    dma = pltpu.SemaphoreType.DMA
    sums = pl.pallas_call(
        kernel,
        out_shape=jax.ShapeDtypeStruct((4, positions.shape[1]), F32),
        in_specs=[vmem, vmem, smem, smem, smem, smem, smem],
        out_specs=vmem,
        scratch_shapes=[
            pltpu.VMEM((2, CHIPS, 4, 8, TILE), F32),
            pltpu.VMEM((8, 4, 8, TILE), F32),
            pltpu.VMEM((2, CHIPS, 8, TILE), F32),
            pltpu.VMEM((2, CHIPS, 8, TILE), F32),
            pltpu.VMEM((8, 8, TILE), F32),
            pltpu.VMEM((16, TILE, 2 * TILE), BF16),
            pltpu.VMEM((64, 16, 4, 8, TILE), F32),
            pltpu.VMEM((64, 16, 8, TILE), F32),
            pltpu.VMEM((8, TILE, TILE), BF16),
            pltpu.VMEM((TILE, TILE), F32),
            pltpu.VMEM((TILE, TILE), F32),
            pltpu.VMEM((256, 8 * SLOTS), BF16),
            pltpu.VMEM((4, 8 * SLOTS, TILE), F32),
            pltpu.VMEM((SLOTS, 16, 4, 8, TILE), F32),
            pltpu.VMEM((2, CHIPS, 8, TILE), F32),
            pltpu.VMEM((CHIPS, 8, TILE), F32),
            pltpu.VMEM((CHIPS, 8, TILE), F32),
            pltpu.VMEM((CHIPS, 8, TILE), F32),
            pltpu.VMEM((2, CHIPS, 4, 8, TILE), F32),
            pltpu.VMEM((CHIPS, 4, 8, TILE), F32),
            pltpu.VMEM((CHIPS, 4, 8, TILE), F32),
            pltpu.VMEM((CHIPS, 4, 8, TILE), F32),
            dma((31,)), dma((2, CHIPS)), dma((7,)), dma((8,)), dma((3,)), dma((3,)),
            dma((15,)), dma((CHIPS,)), dma((15,)), dma((CHIPS,)), dma((7,)), dma((8,)),
            dma((15,)), dma((CHIPS,)),
        ],
        compiler_params=pltpu.CompilerParams(
            collective_id=0, has_side_effects=True, vmem_limit_bytes=54 * 1024 * 1024
        ),
    )(
        positions,
        types.reshape(8, TILE),
        radius_type,
        valence_type,
        bond_depth,
        pair_tiles.reshape(SLOTS, 2).T,
        tile_count,
    )
    component = lax.broadcasted_iota(jnp.int32, sums.shape, 0)
    return jnp.where(component < 3, F32(-6), F32(-1)) * sums


def solution(mesh):
    in_specs = (
        P(None, ("row", "col")),
        P(("row", "col")),
        P(),
        P(),
        P(),
        P("row", "col", None, None),
        P("row", "col"),
    )
    out_specs = P(None, ("row", "col"))
    return jax.shard_map(local, mesh=mesh, in_specs=in_specs, out_specs=out_specs, check_vma=False)
```

```python
import functools

import jax
import jax.numpy as jnp
from jax import lax
from jax.experimental import pallas as pl
from jax.experimental.pallas import tpu as pltpu
from jax.sharding import PartitionSpec as P

TILE = 128
SLOTS = 96
EARLY = 36
CHIPS = 16
VMEM = 56 * 1024 * 1024
MESH = pl.DeviceIdType.MESH
F32 = jnp.float32
BF16 = jnp.bfloat16
LOG2E = 1.4426950408889634


def pieces(value):
    high = value.astype(BF16).astype(F32)
    rest = value - high
    middle = rest.astype(BF16).astype(F32)
    return high, middle, rest - middle


def by_type(types, table):
    value = jnp.full(types.shape, table[0], F32)
    for t in range(1, len(table)):
        value = jnp.where(types == F32(t), table[t], value)
    return value


def kernel(
    pos_in, types_in, radius_in, valence_in, depth_in, tiles_in, count_in, out_ref,
    pos_ref, types_ref, radius_ref, valence_ref, depth_ref, tiles_ref, count_ref, load_sem,
    rows, cols, row_radius, row_u, col_u, pick_ref, wide, wide_u, col_w, buf_a, buf_b, onehot, parts, store,
    coord_part, coord_rx, force_out, force_in, force_sum, force_rx,
    row_send, row_recv, col_send, col_recv, pair_send, pair_recv,
    c_send, c_recv, u_send, u_recv, v_send, v_recv, f_send, f_recv,
):
    r = lax.axis_index("row")
    c = lax.axis_index("col")
    core = lax.rem(c, 2)
    q = c // 2
    z, x = q // 4, lax.rem(q, 4)
    zh, y = r // 4, lax.rem(r, 4)
    other = 1 - core

    def copy(src, dst, send, recv, row, col):
        return pltpu.make_async_remote_copy(
            src_ref=src, dst_ref=dst, send_sem=send, recv_sem=recv,
            device_id=(row, col), device_id_type=MESH,
        )

    chips = [lax.rem(q + k, CHIPS) for k in range(1, CHIPS)]
    rows_of = [lax.rem(r + k, 8) for k in range(1, 8)]

    def device(zz, xx):
        return (zz * 4 + xx) * 2 + core

    far = [lax.rem(z + k, 4) for k in range(1, 4)]
    side = [lax.rem(x + k, 4) for k in range(1, 4)]
    yy = [lax.rem(y + k, 4) for k in range(1, 4)]
    partner = q * 2 + other
    twin = (1 - zh) * 4 + y
    greeted = [(twin, c)]
    greeted += [(r, device(zz, x)) for zz in far]
    greeted += [(r, device(z, xx)) for xx in side]
    greeted += [(zh * 4 + near, c) for near in yy]
    greeted += [(r, partner)]
    barrier = pltpu.get_barrier_semaphore()
    inputs = (pos_in, types_in, radius_in, valence_in, depth_in, tiles_in, count_in)
    locals_ = (pos_ref, types_ref, radius_ref, valence_ref, depth_ref, tiles_ref, count_ref)
    loads = [pltpu.make_async_copy(a, b, load_sem.at[k]) for k, (a, b) in enumerate(zip(inputs, locals_))]
    for load in loads:
        load.start()

    for row, col in greeted:
        pl.semaphore_signal(barrier, inc=1, device_id=(row, col), device_id_type=MESH)

    sub = lax.broadcasted_iota(jnp.int32, (8, TILE), 0)
    blank = jnp.zeros((8, TILE), F32)
    for k in range(8):
        mark = jnp.where(sub == k, F32(1), F32(0))
        for d in range(4):
            column = [mark if 3 * d <= f < 3 * d + 3 else blank for f in range(16)]
            m = d * 8 + k
            at = slice(m % 2 * TILE, m % 2 * TILE + TILE)
            pick_ref[m // 2, :, at] = jnp.concatenate(column, axis=0).astype(BF16)

    for load in loads:
        load.wait()
    own_types = types_ref[...].astype(F32)
    for k in range(8):
        piece = pos_ref[:, k * TILE : (k + 1) * TILE]
        for d in range(3):
            rows[core, q, d, k : k + 1, :] = piece[d : d + 1]
            cols[r, d, k : k + 1, :] = piece[d : d + 1]
    rows[core, q, 3] = own_types
    cols[r, 3] = own_types

    pl.semaphore_wait(barrier, len(greeted))

    started = []

    def go(*args):
        descriptor = copy(*args)
        descriptor.start()
        started.append(descriptor)

    def send_row(origin, row, col, slot):
        block = rows.at[core, origin]
        go(block, block, row_send.at[slot], row_recv.at[core, origin], row, col)

    def send_col(origin, row, slot):
        block = cols.at[origin]
        go(block, block, col_send.at[slot], col_recv.at[origin], row, c)

    send_col(r, twin, 0)
    for k, zz in enumerate(far):
        send_row(q, r, device(zz, x), k)
    for k, xx in enumerate(side):
        send_row(q, r, device(z, xx), 3 + k)
    for k, near in enumerate(yy):
        send_col(r, zh * 4 + near, 1 + k)
    send_row(q, r, partner, 6)

    def row_wait(par, origin):
        block = rows.at[par, origin]
        copy(block, block, row_send.at[0], row_recv.at[par, origin], r, partner).wait_recv()

    def col_wait(origin):
        block = cols.at[origin]
        copy(block, block, col_send.at[0], col_recv.at[origin], twin, c).wait_recv()

    live = count_ref[0, 0]
    lane_at = lax.broadcasted_iota(jnp.int32, (8, TILE), 1)

    def place_of(at, held):
        a = tiles_ref[0, at]
        place = ((a >> 3) & 1) * 128 + (a >> 4) * 8 + (a & 7)
        return jnp.where((lane_at == at) & (at < live), place, held)

    held = lax.fori_loop(0, SLOTS, place_of, jnp.full((8, TILE), -1, jnp.int32))
    match = lax.broadcasted_iota(jnp.int32, (256, TILE), 0) == held[0:1]
    onehot[...] = jnp.where(match, F32(1), F32(0)).astype(BF16)
    for d in range(4):
        parts[d, SLOTS:TILE, :] = jnp.zeros((TILE - SLOTS, TILE), F32)

    radius = [radius_ref[t] * F32(0.5) for t in range(5)]
    valence = [valence_ref[t] for t in range(5)]

    def turn(feats):
        feats = feats + [blank] * (16 - len(feats))
        return jnp.concatenate(feats, axis=0).T.astype(BF16)

    def lanes_of(left, put_block):
        for m in range(16):
            pair = jnp.dot(left, pick_ref[m], preferred_element_type=F32)
            for h in range(2):
                put_block((2 * m + h) // 8, (2 * m + h) % 8, pair[:, h * TILE : (h + 1) * TILE].reshape(16, 8, TILE))

    def widen(g):
        feats = []
        for value in (cols[g, 0], cols[g, 1], cols[g, 2], by_type(cols[g, 3], radius)):
            feats.extend(pieces(value))

        def put_block(d, k, value):
            wide[g * 8 + k, :, d] = value

        lanes_of(turn(feats), put_block)

    for k, zz in enumerate(far):
        origin = zz * 4 + x
        row_wait(core, origin)
        for j, xx in enumerate(side):
            send_row(origin, r, device(z, xx), 7 + 4 * k + j)
        send_row(origin, r, partner, 10 + 4 * k)

    def relay(k, slot):
        for j, xx in enumerate(side):
            origin = lax.rem(z + k, 4) * 4 + xx
            row_wait(core, origin)
            send_row(origin, r, partner, slot + j)

    widen(r)
    col_wait(twin)
    for k, near in enumerate(yy):
        send_col(twin, zh * 4 + near, 4 + k)
    relay(0, 19)

    def near_cols(k, carry):
        origin = zh * 4 + lax.rem(y + k, 4)
        col_wait(origin)
        widen(origin)
        return carry

    lax.fori_loop(1, 4, near_cols, 0)
    for k in range(1, 4):
        relay(k, 19 + 3 * k)
    widen(twin)

    def far_cols(k, carry):
        origin = (1 - zh) * 4 + lax.rem(y + k, 4)
        col_wait(origin)
        widen(origin)
        return carry

    lax.fori_loop(1, 4, far_cols, 0)
    for p in range(CHIPS):
        row_wait(other, p)
    for par in range(2):
        for p in range(CHIPS):
            row_radius[par, p] = by_type(rows[par, p, 3], radius)

    def tile_of(s):
        a = tiles_ref[0, s]
        b = tiles_ref[1, s]
        return (a >> 3) & 1, a >> 4, a & 7, b

    def same_block(s):
        a = tiles_ref[0, s]
        b = tiles_ref[1, s]
        same = ((b >> 3) == r) & ((a >> 3) == c) & ((a & 7) == (b & 7))
        return jnp.where(same, F32(1), F32(0))

    def near_rows(s):
        sp, sq, sb, b = tile_of(s)
        near = [rows[sp, sq, d, pl.ds(sb, 1), :] for d in range(3)]
        return near, row_radius[sp, sq, pl.ds(sb, 1), :], b

    def over_tiles(fill, use, begin, end):
        fill(begin, buf_a)

        def body(t, carry):
            s = begin + 2 * t
            fill(s + 1, buf_b)
            use(s, buf_a)
            fill(jnp.minimum(s + 2, SLOTS - 1), buf_a)
            use(s + 1, buf_b)
            return carry

        lax.fori_loop(0, (end - begin) // 2, body, 0)

    def put(d, s, value):
        parts[d, pl.ds(s, 1), :] = jnp.sum(value, axis=0, keepdims=True)

    def first(s):
        near, near_r, b = near_rows(s)
        total = jnp.where(sub == 0, -same_block(s), F32(0))
        for k in range(16):
            dist = F32(0)
            for d in range(3):
                offset = near[d] - wide[b, k, d]
                dist = dist + offset * offset
            rho = near_r + wide[b, k, 3]
            ratio = dist / (rho * rho)
            total = total + jnp.exp2((ratio * ratio) * (ratio * F32(-LOG2E)))
        put(0, s, total)

    def by_fours(use):
        def body(t, carry):
            for k in range(4):
                use(4 * t + k)
            return carry

        lax.fori_loop(0, SLOTS // 4, body, 0)

    by_fours(first)

    def scatter(value):
        high = value.astype(BF16)
        low = (value - high.astype(F32)).astype(BF16)
        return high, low

    def spots(value):
        return value.reshape(2, CHIPS, 8, TILE)

    both = jnp.concatenate(scatter(parts[0]), axis=1)
    both = jnp.dot(onehot[...], both, preferred_element_type=F32)
    coord_part[...] = spots(both[:, :TILE] + both[:, TILE:])
    peers = [(par, p) for p in chips for par in (core, other)] + [(other, q)]
    for k, (par, p) in enumerate(peers):
        go(coord_part.at[par, p], coord_rx.at[core, q], c_send.at[k], c_recv.at[core, q], r, p * 2 + par)

    for g in range(8):
        feats = []
        for t in range(5):
            table = [depth_ref[t, u] * (valence[t] + valence[u]) for u in range(5)]
            feats.extend(pieces(by_type(cols[g, 3], table)))
        col_w[g] = turn(feats)

    def pair_terms(s, buf):
        sp, sq, sb, b = tile_of(s)
        kinds = jnp.broadcast_to(rows[sp, sq, 3, pl.ds(sb, 1), :], (8, TILE))
        kinds = jnp.where(sub == (b & 7), kinds, F32(-1))
        right = []
        for t in range(5):
            right.extend([jnp.where(kinds == F32(t), F32(1), F32(0))] * 3)
        right = jnp.concatenate(right + [blank], axis=0).astype(BF16)
        buf[...] = jnp.dot(col_w[b >> 3], right, preferred_element_type=F32)

    def prepare(s, buf):
        near, near_r, b = near_rows(s)
        same = same_block(s)
        for k in range(16):
            dx, dy, dz = (near[d] - wide[b, k, d] for d in range(3))
            rho = near_r + wide[b, k, 3]
            inverse = F32(1) / (rho * rho)
            ratio = (dx * dx + dy * dy + dz * dz) * inverse
            square = ratio * ratio
            numer = buf[8 * k : 8 * k + 8, :] * jnp.exp2(square * (ratio * F32(-LOG2E)))
            numer = jnp.where(lane_at == sub + 8 * k, numer * (F32(1) - same), numer)
            pull = numer * (square * inverse)
            store[s, k, 0] = pull * dx
            store[s, k, 1] = pull * dy
            store[s, k, 2] = pull * dz
            store[s, k, 3] = numer

    over_tiles(pair_terms, prepare, 0, EARLY)

    own = coord_part[core, q]
    for par, p in peers:
        block = coord_rx.at[par, p]
        copy(block, block, c_send.at[0], c_recv.at[par, p], r, p * 2 + par).wait_recv()
        own = own + coord_rx[par, p]
    own = own + by_type(rows[core, q, 3], valence)
    row_u[core, q] = own
    col_u[r] = own
    for k, p in enumerate(rows_of):
        go(col_u.at[r], col_u.at[r], v_send.at[k], v_recv.at[r], p, c)
    for k, p in enumerate(chips):
        go(row_u.at[core, q], row_u.at[core, q], u_send.at[k], u_recv.at[q], r, p * 2 + core)

    over_tiles(pair_terms, prepare, EARLY, SLOTS)

    for p in chips:
        block = row_u.at[core, p]
        copy(block, block, u_send.at[0], u_recv.at[p], r, p * 2 + core).wait_recv()
    go(row_u.at[core], row_u.at[core], pair_send.at[1], pair_recv.at[1], r, partner)
    for side_of in (zh, 1 - zh):
        for k in range(4):
            p = side_of * 4 + lax.rem(y + k, 4)
            if side_of is zh and k == 0:
                continue
            copy(col_u.at[p], col_u.at[p], v_send.at[0], v_recv.at[p], p, c).wait_recv()
        feats = []
        for k in range(4):
            feats.extend(pieces(col_u[4 * side_of + k]))

        def put_u(d, k, value, side_of=side_of):
            wide_u[side_of * 32 + d * 8 + k] = value

        lanes_of(turn(feats), put_u)
    copy(row_u.at[other], row_u.at[other], pair_send.at[1], pair_recv.at[1], r, partner).wait_recv()

    def second(s):
        sp, sq, sb, b = tile_of(s)
        near = row_u[sp, sq, pl.ds(sb, 1), :]
        total = [F32(0)] * 4
        for k in range(16):
            scale = F32(1) / (near + wide_u[b, k])
            for d in range(4):
                total[d] = total[d] + store[s, k, d] * scale
        for d in range(4):
            put(d, s, total[d])

    by_fours(second)

    sums = [scatter(jnp.concatenate([parts[d], parts[d + 1]], axis=1)) for d in (0, 2)]

    def gathered(par, ref):
        chosen = onehot[pl.ds(pl.multiple_of(par * TILE, TILE), TILE), :]
        for d, (high, low) in zip((0, 2), sums):
            both = jnp.dot(chosen, high, preferred_element_type=F32)
            both = both + jnp.dot(chosen, low, preferred_element_type=F32)
            ref[:, d] = both[:, :TILE].reshape(CHIPS, 8, TILE)
            ref[:, d + 1] = both[:, TILE:].reshape(CHIPS, 8, TILE)

    gathered(other, force_out)
    go(force_out, force_in, pair_send.at[2], pair_recv.at[2], r, partner)
    gathered(core, force_sum)
    copy(force_out, force_in, pair_send.at[2], pair_recv.at[2], r, partner).wait_recv()
    force_sum[...] = force_sum[...] + force_in[...]
    for k, p in enumerate(chips):
        go(force_sum.at[p], force_rx.at[q], f_send.at[k], f_recv.at[q], r, p * 2 + core)
    own = force_sum[q]
    for p in chips:
        copy(force_sum.at[0], force_rx.at[p], f_send.at[0], f_recv.at[p], r, p * 2 + core).wait_recv()
        own = own + force_rx[p]
    for k in range(8):
        out_ref[:, k * TILE : (k + 1) * TILE] = own[:, k, :]
    for descriptor in started:
        descriptor.wait_send()


def local(positions, types, radius_type, valence_type, bond_depth, pair_tiles, tile_count):
    vmem = pl.BlockSpec(memory_space=pltpu.VMEM)
    smem = pltpu.SMEM
    dma = pltpu.SemaphoreType.DMA
    sums = pl.pallas_call(
        kernel,
        out_shape=jax.ShapeDtypeStruct((4, positions.shape[1]), F32),
        in_specs=[pl.BlockSpec(memory_space=pltpu.HBM)] * 7,
        out_specs=vmem,
        scratch_shapes=[
            pltpu.VMEM(positions.shape, F32),
            pltpu.VMEM((8, TILE), jnp.int32),
            smem(radius_type.shape, F32),
            smem(valence_type.shape, F32),
            smem(bond_depth.shape, F32),
            smem((2, SLOTS), jnp.int32),
            smem((1, 1), jnp.int32),
            dma((7,)),
            pltpu.VMEM((2, CHIPS, 4, 8, TILE), F32),
            pltpu.VMEM((8, 4, 8, TILE), F32),
            pltpu.VMEM((2, CHIPS, 8, TILE), F32),
            pltpu.VMEM((2, CHIPS, 8, TILE), F32),
            pltpu.VMEM((8, 8, TILE), F32),
            pltpu.VMEM((16, TILE, 2 * TILE), BF16),
            pltpu.VMEM((64, 16, 4, 8, TILE), F32),
            pltpu.VMEM((64, 16, 8, TILE), F32),
            pltpu.VMEM((8, TILE, TILE), BF16),
            pltpu.VMEM((TILE, TILE), F32),
            pltpu.VMEM((TILE, TILE), F32),
            pltpu.VMEM((256, TILE), BF16),
            pltpu.VMEM((4, TILE, TILE), F32),
            pltpu.VMEM((SLOTS, 16, 4, 8, TILE), F32),
            pltpu.VMEM((2, CHIPS, 8, TILE), F32),
            pltpu.VMEM((2, CHIPS, 8, TILE), F32),
            pltpu.VMEM((CHIPS, 4, 8, TILE), F32),
            pltpu.VMEM((CHIPS, 4, 8, TILE), F32),
            pltpu.VMEM((CHIPS, 4, 8, TILE), F32),
            pltpu.VMEM((CHIPS, 4, 8, TILE), F32),
            dma((31,)), dma((2, CHIPS)), dma((7,)), dma((8,)), dma((3,)), dma((3,)),
            dma((31,)), dma((2, CHIPS)), dma((15,)), dma((CHIPS,)), dma((7,)), dma((8,)),
            dma((15,)), dma((CHIPS,)),
        ],
        compiler_params=pltpu.CompilerParams(
            collective_id=0, has_side_effects=True, vmem_limit_bytes=VMEM
        ),
    )(
        positions,
        types.reshape(8, TILE),
        radius_type,
        valence_type,
        bond_depth,
        pair_tiles.reshape(SLOTS, 2).T,
        tile_count,
    )
    component = lax.broadcasted_iota(jnp.int32, sums.shape, 0)
    return jnp.where(component < 3, F32(-6), F32(-1)) * sums


def solution(mesh):
    in_specs = (
        P(None, ("row", "col")),
        P(("row", "col")),
        P(),
        P(),
        P(),
        P("row", "col", None, None),
        P("row", "col"),
    )
    out_specs = P(None, ("row", "col"))
    return jax.shard_map(local, mesh=mesh, in_specs=in_specs, out_specs=out_specs, check_vma=False)
```

```python
import functools

import jax
import jax.numpy as jnp
from jax import lax
from jax.experimental import pallas as pl
from jax.experimental.pallas import tpu as pltpu
from jax.sharding import PartitionSpec as P

TILE = 128
SLOTS = 96
EARLY = 36
CHIPS = 16
VMEM = 56 * 1024 * 1024
MESH = pl.DeviceIdType.MESH
F32 = jnp.float32
BF16 = jnp.bfloat16
LOG2E = 1.4426950408889634


def pieces(value):
    high = value.astype(BF16).astype(F32)
    rest = value - high
    middle = rest.astype(BF16).astype(F32)
    return high, middle, rest - middle


def by_type(types, table):
    value = jnp.full(types.shape, table[0], F32)
    for t in range(1, len(table)):
        value = jnp.where(types == F32(t), table[t], value)
    return value


def kernel(
    pos_in, types_in, radius_in, valence_in, depth_in, tiles_in, count_in, out_ref,
    pos_ref, types_ref, radius_ref, valence_ref, depth_ref, tiles_ref, count_ref, load_sem,
    rows, cols, row_radius, row_u, col_u, pick_ref, wide, wide_u, col_w, buf_a, buf_b, onehot, parts, store,
    coord_part, coord_rx, force_out, force_in, force_sum, force_rx,
    row_send, row_recv, col_send, col_recv, pair_send, pair_recv,
    c_send, c_recv, u_send, u_recv, v_send, v_recv, f_send, f_recv,
):
    r = lax.axis_index("row")
    c = lax.axis_index("col")
    core = lax.rem(c, 2)
    q = c // 2
    z, x = q // 4, lax.rem(q, 4)
    zh, y = r // 4, lax.rem(r, 4)
    other = 1 - core

    def copy(src, dst, send, recv, row, col):
        return pltpu.make_async_remote_copy(
            src_ref=src, dst_ref=dst, send_sem=send, recv_sem=recv,
            device_id=(row, col), device_id_type=MESH,
        )

    chips = [lax.rem(q + k, CHIPS) for k in range(1, CHIPS)]
    rows_of = [lax.rem(r + k, 8) for k in range(1, 8)]

    def device(zz, xx):
        return (zz * 4 + xx) * 2 + core

    half = z // 2
    far = [z + 1 - 2 * lax.rem(z, 2), 2 - half, 3 * (1 - half)]
    side = [lax.rem(x + k, 4) for k in range(1, 4)]
    yy = [lax.rem(y + k, 4) for k in range(1, 4)]
    partner = q * 2 + other
    twin = (1 - zh) * 4 + y
    greeted = [(twin, c)]
    greeted += [(r, device(zz, x)) for zz in far]
    greeted += [(r, device(z, xx)) for xx in side]
    greeted += [(zh * 4 + near, c) for near in yy]
    greeted += [(r, partner)]
    barrier = pltpu.get_barrier_semaphore()
    inputs = (pos_in, types_in, radius_in, valence_in, depth_in, tiles_in, count_in)
    locals_ = (pos_ref, types_ref, radius_ref, valence_ref, depth_ref, tiles_ref, count_ref)
    loads = [pltpu.make_async_copy(a, b, load_sem.at[k]) for k, (a, b) in enumerate(zip(inputs, locals_))]
    for load in loads:
        load.start()

    for row, col in greeted:
        pl.semaphore_signal(barrier, inc=1, device_id=(row, col), device_id_type=MESH)

    sub = lax.broadcasted_iota(jnp.int32, (8, TILE), 0)
    blank = jnp.zeros((8, TILE), F32)
    for k in range(8):
        mark = jnp.where(sub == k, F32(1), F32(0))
        for d in range(4):
            column = [mark if 3 * d <= f < 3 * d + 3 else blank for f in range(16)]
            m = d * 8 + k
            at = slice(m % 2 * TILE, m % 2 * TILE + TILE)
            pick_ref[m // 2, :, at] = jnp.concatenate(column, axis=0).astype(BF16)

    for load in loads:
        load.wait()
    own_types = types_ref[...].astype(F32)
    for k in range(8):
        piece = pos_ref[:, k * TILE : (k + 1) * TILE]
        for d in range(3):
            rows[core, q, d, k : k + 1, :] = piece[d : d + 1]
            cols[r, d, k : k + 1, :] = piece[d : d + 1]
    rows[core, q, 3] = own_types
    cols[r, 3] = own_types

    pl.semaphore_wait(barrier, len(greeted))

    started = []

    def go(*args):
        descriptor = copy(*args)
        descriptor.start()
        started.append(descriptor)

    def send_row(origin, row, col, slot):
        block = rows.at[core, origin]
        go(block, block, row_send.at[slot], row_recv.at[core, origin], row, col)

    def send_col(origin, row, slot):
        block = cols.at[origin]
        go(block, block, col_send.at[slot], col_recv.at[origin], row, c)

    send_col(r, twin, 0)
    for k, zz in enumerate(far[::-1]):
        send_row(q, r, device(zz, x), k)
    for k, xx in enumerate(side):
        send_row(q, r, device(z, xx), 3 + k)
    for k, near in enumerate(yy):
        send_col(r, zh * 4 + near, 1 + k)
    send_row(q, r, partner, 6)

    def row_wait(par, origin):
        block = rows.at[par, origin]
        copy(block, block, row_send.at[0], row_recv.at[par, origin], r, partner).wait_recv()

    def col_wait(origin):
        block = cols.at[origin]
        copy(block, block, col_send.at[0], col_recv.at[origin], twin, c).wait_recv()

    live = count_ref[0, 0]
    lane_at = lax.broadcasted_iota(jnp.int32, (8, TILE), 1)

    def place_of(at, held):
        a = tiles_ref[0, at]
        place = ((a >> 3) & 1) * 128 + (a >> 4) * 8 + (a & 7)
        return jnp.where((lane_at == at) & (at < live), place, held)

    held = lax.fori_loop(0, SLOTS, place_of, jnp.full((8, TILE), -1, jnp.int32))
    match = lax.broadcasted_iota(jnp.int32, (256, TILE), 0) == held[0:1]
    onehot[...] = jnp.where(match, F32(1), F32(0)).astype(BF16)
    for d in range(4):
        parts[d, SLOTS:TILE, :] = jnp.zeros((TILE - SLOTS, TILE), F32)

    radius = [radius_ref[t] * F32(0.5) for t in range(5)]
    valence = [valence_ref[t] for t in range(5)]

    def turn(feats):
        feats = feats + [blank] * (16 - len(feats))
        return jnp.concatenate(feats, axis=0).T.astype(BF16)

    def lanes_of(left, put_block):
        for m in range(16):
            pair = jnp.dot(left, pick_ref[m], preferred_element_type=F32)
            for h in range(2):
                put_block((2 * m + h) // 8, (2 * m + h) % 8, pair[:, h * TILE : (h + 1) * TILE].reshape(16, 8, TILE))

    def widen(g):
        feats = []
        for value in (cols[g, 0], cols[g, 1], cols[g, 2], by_type(cols[g, 3], radius)):
            feats.extend(pieces(value))

        def put_block(d, k, value):
            wide[g * 8 + k, :, d] = value

        lanes_of(turn(feats), put_block)

    for k, zz in enumerate(far):
        origin = zz * 4 + x
        row_wait(core, origin)
        for j, xx in enumerate(side):
            send_row(origin, r, device(z, xx), 7 + 4 * k + j)
        send_row(origin, r, partner, 10 + 4 * k)

    def relay(k, slot):
        for j, xx in enumerate(side):
            origin = [z, *far][k] * 4 + xx
            row_wait(core, origin)
            send_row(origin, r, partner, slot + j)

    widen(r)
    col_wait(twin)
    for k, near in enumerate(yy):
        send_col(twin, zh * 4 + near, 4 + k)
    relay(0, 19)

    def near_cols(k, carry):
        origin = zh * 4 + lax.rem(y + k, 4)
        col_wait(origin)
        widen(origin)
        return carry

    lax.fori_loop(1, 4, near_cols, 0)
    for k in range(1, 4):
        relay(k, 19 + 3 * k)
    widen(twin)

    def far_cols(k, carry):
        origin = (1 - zh) * 4 + lax.rem(y + k, 4)
        col_wait(origin)
        widen(origin)
        return carry

    lax.fori_loop(1, 4, far_cols, 0)
    for p in range(CHIPS):
        row_wait(other, p)
    for par in range(2):
        for p in range(CHIPS):
            row_radius[par, p] = by_type(rows[par, p, 3], radius)

    def tile_of(s):
        a = tiles_ref[0, s]
        b = tiles_ref[1, s]
        return (a >> 3) & 1, a >> 4, a & 7, b

    def same_block(s):
        a = tiles_ref[0, s]
        b = tiles_ref[1, s]
        same = ((b >> 3) == r) & ((a >> 3) == c) & ((a & 7) == (b & 7))
        return jnp.where(same, F32(1), F32(0))

    def near_rows(s):
        sp, sq, sb, b = tile_of(s)
        near = [rows[sp, sq, d, pl.ds(sb, 1), :] for d in range(3)]
        return near, row_radius[sp, sq, pl.ds(sb, 1), :], b

    def over_tiles(fill, use, begin, end):
        fill(begin, buf_a)

        def body(t, carry):
            s = begin + 2 * t
            fill(s + 1, buf_b)
            use(s, buf_a)
            fill(jnp.minimum(s + 2, SLOTS - 1), buf_a)
            use(s + 1, buf_b)
            return carry

        lax.fori_loop(0, (end - begin) // 2, body, 0)

    def put(d, s, value):
        parts[d, pl.ds(s, 1), :] = jnp.sum(value, axis=0, keepdims=True)

    def first(s):
        near, near_r, b = near_rows(s)
        total = jnp.where(sub == 0, -same_block(s), F32(0))
        for k in range(16):
            dist = F32(0)
            for d in range(3):
                offset = near[d] - wide[b, k, d]
                dist = dist + offset * offset
            rho = near_r + wide[b, k, 3]
            ratio = dist / (rho * rho)
            total = total + jnp.exp2((ratio * ratio) * (ratio * F32(-LOG2E)))
        put(0, s, total)

    def by_fours(use):
        def body(t, carry):
            for k in range(4):
                use(4 * t + k)
            return carry

        lax.fori_loop(0, SLOTS // 4, body, 0)

    by_fours(first)

    def scatter(value):
        high = value.astype(BF16)
        low = (value - high.astype(F32)).astype(BF16)
        return high, low

    def spots(value):
        return value.reshape(2, CHIPS, 8, TILE)

    both = jnp.concatenate(scatter(parts[0]), axis=1)
    both = jnp.dot(onehot[...], both, preferred_element_type=F32)
    coord_part[...] = spots(both[:, :TILE] + both[:, TILE:])
    peers = [(par, p) for p in chips for par in (core, other)] + [(other, q)]
    for k, (par, p) in enumerate(peers):
        go(coord_part.at[par, p], coord_rx.at[core, q], c_send.at[k], c_recv.at[core, q], r, p * 2 + par)

    for g in range(8):
        feats = []
        for t in range(5):
            table = [depth_ref[t, u] * (valence[t] + valence[u]) for u in range(5)]
            feats.extend(pieces(by_type(cols[g, 3], table)))
        col_w[g] = turn(feats)

    def pair_terms(s, buf):
        sp, sq, sb, b = tile_of(s)
        kinds = jnp.broadcast_to(rows[sp, sq, 3, pl.ds(sb, 1), :], (8, TILE))
        kinds = jnp.where(sub == (b & 7), kinds, F32(-1))
        right = []
        for t in range(5):
            right.extend([jnp.where(kinds == F32(t), F32(1), F32(0))] * 3)
        right = jnp.concatenate(right + [blank], axis=0).astype(BF16)
        buf[...] = jnp.dot(col_w[b >> 3], right, preferred_element_type=F32)

    def prepare(s, buf):
        near, near_r, b = near_rows(s)
        same = same_block(s)
        for k in range(16):
            dx, dy, dz = (near[d] - wide[b, k, d] for d in range(3))
            rho = near_r + wide[b, k, 3]
            inverse = F32(1) / (rho * rho)
            ratio = (dx * dx + dy * dy + dz * dz) * inverse
            square = ratio * ratio
            numer = buf[8 * k : 8 * k + 8, :] * jnp.exp2(square * (ratio * F32(-LOG2E)))
            numer = jnp.where(lane_at == sub + 8 * k, numer * (F32(1) - same), numer)
            pull = numer * (square * inverse)
            store[s, k, 0] = pull * dx
            store[s, k, 1] = pull * dy
            store[s, k, 2] = pull * dz
            store[s, k, 3] = numer

    over_tiles(pair_terms, prepare, 0, EARLY)

    own = coord_part[core, q]
    for par, p in peers:
        block = coord_rx.at[par, p]
        copy(block, block, c_send.at[0], c_recv.at[par, p], r, p * 2 + par).wait_recv()
        own = own + coord_rx[par, p]
    own = own + by_type(rows[core, q, 3], valence)
    row_u[core, q] = own
    col_u[r] = own
    for k, p in enumerate(rows_of):
        go(col_u.at[r], col_u.at[r], v_send.at[k], v_recv.at[r], p, c)
    for k, p in enumerate(chips):
        go(row_u.at[core, q], row_u.at[core, q], u_send.at[k], u_recv.at[q], r, p * 2 + core)

    over_tiles(pair_terms, prepare, EARLY, SLOTS)

    for p in chips:
        block = row_u.at[core, p]
        copy(block, block, u_send.at[0], u_recv.at[p], r, p * 2 + core).wait_recv()
    go(row_u.at[core], row_u.at[core], pair_send.at[1], pair_recv.at[1], r, partner)
    for side_of in (zh, 1 - zh):
        for k in range(4):
            p = side_of * 4 + lax.rem(y + k, 4)
            if side_of is zh and k == 0:
                continue
            copy(col_u.at[p], col_u.at[p], v_send.at[0], v_recv.at[p], p, c).wait_recv()
        feats = []
        for k in range(4):
            feats.extend(pieces(col_u[4 * side_of + k]))

        def put_u(d, k, value, side_of=side_of):
            wide_u[side_of * 32 + d * 8 + k] = value

        lanes_of(turn(feats), put_u)
    copy(row_u.at[other], row_u.at[other], pair_send.at[1], pair_recv.at[1], r, partner).wait_recv()

    def second(s):
        sp, sq, sb, b = tile_of(s)
        near = row_u[sp, sq, pl.ds(sb, 1), :]
        total = [F32(0)] * 4
        for k in range(16):
            scale = F32(1) / (near + wide_u[b, k])
            for d in range(4):
                total[d] = total[d] + store[s, k, d] * scale
        for d in range(4):
            put(d, s, total[d])

    by_fours(second)

    sums = [scatter(jnp.concatenate([parts[d], parts[d + 1]], axis=1)) for d in (0, 2)]

    def gathered(par, ref):
        chosen = onehot[pl.ds(pl.multiple_of(par * TILE, TILE), TILE), :]
        for d, (high, low) in zip((0, 2), sums):
            both = jnp.dot(chosen, high, preferred_element_type=F32)
            both = both + jnp.dot(chosen, low, preferred_element_type=F32)
            ref[:, d] = both[:, :TILE].reshape(CHIPS, 8, TILE)
            ref[:, d + 1] = both[:, TILE:].reshape(CHIPS, 8, TILE)

    gathered(other, force_out)
    go(force_out, force_in, pair_send.at[2], pair_recv.at[2], r, partner)
    gathered(core, force_sum)
    copy(force_out, force_in, pair_send.at[2], pair_recv.at[2], r, partner).wait_recv()
    force_sum[...] = force_sum[...] + force_in[...]
    for k, p in enumerate(chips):
        go(force_sum.at[p], force_rx.at[q], f_send.at[k], f_recv.at[q], r, p * 2 + core)
    own = force_sum[q]
    for p in chips:
        copy(force_sum.at[0], force_rx.at[p], f_send.at[0], f_recv.at[p], r, p * 2 + core).wait_recv()
        own = own + force_rx[p]
    for k in range(8):
        out_ref[:, k * TILE : (k + 1) * TILE] = own[:, k, :]
    for descriptor in started:
        descriptor.wait_send()


def local(positions, types, radius_type, valence_type, bond_depth, pair_tiles, tile_count):
    vmem = pl.BlockSpec(memory_space=pltpu.VMEM)
    smem = pltpu.SMEM
    dma = pltpu.SemaphoreType.DMA
    sums = pl.pallas_call(
        kernel,
        out_shape=jax.ShapeDtypeStruct((4, positions.shape[1]), F32),
        in_specs=[pl.BlockSpec(memory_space=pltpu.HBM)] * 7,
        out_specs=vmem,
        scratch_shapes=[
            pltpu.VMEM(positions.shape, F32),
            pltpu.VMEM((8, TILE), jnp.int32),
            smem(radius_type.shape, F32),
            smem(valence_type.shape, F32),
            smem(bond_depth.shape, F32),
            smem((2, SLOTS), jnp.int32),
            smem((1, 1), jnp.int32),
            dma((7,)),
            pltpu.VMEM((2, CHIPS, 4, 8, TILE), F32),
            pltpu.VMEM((8, 4, 8, TILE), F32),
            pltpu.VMEM((2, CHIPS, 8, TILE), F32),
            pltpu.VMEM((2, CHIPS, 8, TILE), F32),
            pltpu.VMEM((8, 8, TILE), F32),
            pltpu.VMEM((16, TILE, 2 * TILE), BF16),
            pltpu.VMEM((64, 16, 4, 8, TILE), F32),
            pltpu.VMEM((64, 16, 8, TILE), F32),
            pltpu.VMEM((8, TILE, TILE), BF16),
            pltpu.VMEM((TILE, TILE), F32),
            pltpu.VMEM((TILE, TILE), F32),
            pltpu.VMEM((256, TILE), BF16),
            pltpu.VMEM((4, TILE, TILE), F32),
            pltpu.VMEM((SLOTS, 16, 4, 8, TILE), F32),
            pltpu.VMEM((2, CHIPS, 8, TILE), F32),
            pltpu.VMEM((2, CHIPS, 8, TILE), F32),
            pltpu.VMEM((CHIPS, 4, 8, TILE), F32),
            pltpu.VMEM((CHIPS, 4, 8, TILE), F32),
            pltpu.VMEM((CHIPS, 4, 8, TILE), F32),
            pltpu.VMEM((CHIPS, 4, 8, TILE), F32),
            dma((31,)), dma((2, CHIPS)), dma((7,)), dma((8,)), dma((3,)), dma((3,)),
            dma((31,)), dma((2, CHIPS)), dma((15,)), dma((CHIPS,)), dma((7,)), dma((8,)),
            dma((15,)), dma((CHIPS,)),
        ],
        compiler_params=pltpu.CompilerParams(
            collective_id=0, has_side_effects=True, vmem_limit_bytes=VMEM
        ),
    )(
        positions,
        types.reshape(8, TILE),
        radius_type,
        valence_type,
        bond_depth,
        pair_tiles.reshape(SLOTS, 2).T,
        tile_count,
    )
    component = lax.broadcasted_iota(jnp.int32, sums.shape, 0)
    return jnp.where(component < 3, F32(-6), F32(-1)) * sums


def solution(mesh):
    in_specs = (
        P(None, ("row", "col")),
        P(("row", "col")),
        P(),
        P(),
        P(),
        P("row", "col", None, None),
        P("row", "col"),
    )
    out_specs = P(None, ("row", "col"))
    return jax.shard_map(local, mesh=mesh, in_specs=in_specs, out_specs=out_specs, check_vma=False)
```

```python
import functools

import jax
import jax.numpy as jnp
from jax import lax
from jax.experimental import pallas as pl
from jax.experimental.pallas import tpu as pltpu
from jax.sharding import PartitionSpec as P

TILE = 128
SLOTS = 96
EARLY = 36
CHIPS = 16
VMEM = 56 * 1024 * 1024
MESH = pl.DeviceIdType.MESH
F32 = jnp.float32
BF16 = jnp.bfloat16
LOG2E = 1.4426950408889634


def pieces(value):
    high = value.astype(BF16).astype(F32)
    rest = value - high
    middle = rest.astype(BF16).astype(F32)
    return high, middle, rest - middle


def by_type(types, table):
    value = jnp.full(types.shape, table[0], F32)
    for t in range(1, len(table)):
        value = jnp.where(types == F32(t), table[t], value)
    return value


def kernel(
    pos_in, types_in, radius_in, valence_in, depth_in, tiles_in, count_in, out_ref,
    pos_ref, types_ref, radius_ref, valence_ref, depth_ref, tiles_ref, count_ref, load_sem,
    rows, cols, row_radius, row_u, col_u, pick_ref, wide, wide_u, col_w, buf_a, buf_b, onehot, parts, store,
    coord_part, coord_rx, force_out, force_in, force_sum, force_rx,
    row_send, row_recv, col_send, col_recv, pair_send, pair_recv,
    c_send, c_recv, u_send, u_recv, v_send, v_recv, f_send, f_recv,
):
    r = lax.axis_index("row")
    c = lax.axis_index("col")
    core = lax.rem(c, 2)
    q = c // 2
    z, x = q // 4, lax.rem(q, 4)
    zh, y = r // 4, lax.rem(r, 4)
    other = 1 - core

    def copy(src, dst, send, recv, row, col):
        return pltpu.make_async_remote_copy(
            src_ref=src, dst_ref=dst, send_sem=send, recv_sem=recv,
            device_id=(row, col), device_id_type=MESH,
        )

    chips = [lax.rem(q + k, CHIPS) for k in range(1, CHIPS)]
    rows_of = [lax.rem(r + k, 8) for k in range(1, 8)]

    def device(zz, xx):
        return (zz * 4 + xx) * 2 + core

    half = z // 2
    far = [z + 1 - 2 * lax.rem(z, 2), 2 - half, 3 * (1 - half)]
    side = [lax.rem(x + k, 4) for k in range(1, 4)]
    yy = [lax.rem(y + k, 4) for k in range(1, 4)]
    partner = q * 2 + other
    twin = (1 - zh) * 4 + y
    greeted = [(twin, c)]
    greeted += [(r, device(zz, x)) for zz in far]
    greeted += [(r, device(z, xx)) for xx in side]
    greeted += [(zh * 4 + near, c) for near in yy]
    greeted += [(r, partner)]
    barrier = pltpu.get_barrier_semaphore()
    inputs = (pos_in, types_in, radius_in, valence_in, depth_in, tiles_in, count_in)
    locals_ = (pos_ref, types_ref, radius_ref, valence_ref, depth_ref, tiles_ref, count_ref)
    loads = [pltpu.make_async_copy(a, b, load_sem.at[k]) for k, (a, b) in enumerate(zip(inputs, locals_))]
    for load in loads:
        load.start()

    for row, col in greeted:
        pl.semaphore_signal(barrier, inc=1, device_id=(row, col), device_id_type=MESH)

    sub = lax.broadcasted_iota(jnp.int32, (8, TILE), 0)
    blank = jnp.zeros((8, TILE), F32)
    for k in range(8):
        mark = jnp.where(sub == k, F32(1), F32(0))
        for d in range(4):
            column = [mark if 3 * d <= f < 3 * d + 3 else blank for f in range(16)]
            m = d * 8 + k
            at = slice(m % 2 * TILE, m % 2 * TILE + TILE)
            pick_ref[m // 2, :, at] = jnp.concatenate(column, axis=0).astype(BF16)

    for load in loads:
        load.wait()
    own_types = types_ref[...].astype(F32)
    for k in range(8):
        piece = pos_ref[:, k * TILE : (k + 1) * TILE]
        for d in range(3):
            rows[core, q, d, k : k + 1, :] = piece[d : d + 1]
            cols[r, d, k : k + 1, :] = piece[d : d + 1]
    rows[core, q, 3] = own_types
    cols[r, 3] = own_types

    pl.semaphore_wait(barrier, len(greeted))

    started = []

    def go(*args):
        descriptor = copy(*args)
        descriptor.start()
        started.append(descriptor)

    def send_row(origin, row, col, slot):
        block = rows.at[core, origin]
        go(block, block, row_send.at[slot], row_recv.at[core, origin], row, col)

    def send_col(origin, row, slot):
        block = cols.at[origin]
        go(block, block, col_send.at[slot], col_recv.at[origin], row, c)

    send_col(r, twin, 0)
    for k, zz in enumerate(far[::-1]):
        send_row(q, r, device(zz, x), k)
    for k, xx in enumerate(side):
        send_row(q, r, device(z, xx), 3 + k)
    for k, near in enumerate(yy):
        send_col(r, zh * 4 + near, 1 + k)
    send_row(q, r, partner, 6)

    def row_wait(par, origin):
        block = rows.at[par, origin]
        copy(block, block, row_send.at[0], row_recv.at[par, origin], r, partner).wait_recv()

    def col_wait(origin):
        block = cols.at[origin]
        copy(block, block, col_send.at[0], col_recv.at[origin], twin, c).wait_recv()

    live = count_ref[0, 0]
    lane_at = lax.broadcasted_iota(jnp.int32, (8, TILE), 1)

    def place_of(at, held):
        a = tiles_ref[0, at]
        place = ((a >> 3) & 1) * 128 + (a >> 4) * 8 + (a & 7)
        return jnp.where((lane_at == at) & (at < live), place, held)

    held = lax.fori_loop(0, SLOTS, place_of, jnp.full((8, TILE), -1, jnp.int32))
    match = lax.broadcasted_iota(jnp.int32, (256, TILE), 0) == held[0:1]
    onehot[...] = jnp.where(match, F32(1), F32(0)).astype(BF16)
    for d in range(4):
        parts[d, SLOTS:TILE, :] = jnp.zeros((TILE - SLOTS, TILE), F32)

    radius = [radius_ref[t] * F32(0.5) for t in range(5)]
    valence = [valence_ref[t] for t in range(5)]

    def turn(feats):
        feats = feats + [blank] * (16 - len(feats))
        return jnp.concatenate(feats, axis=0).T.astype(BF16)

    def lanes_of(left, put_block):
        for m in range(16):
            pair = jnp.dot(left, pick_ref[m], preferred_element_type=F32)
            for h in range(2):
                put_block((2 * m + h) // 8, (2 * m + h) % 8, pair[:, h * TILE : (h + 1) * TILE].reshape(16, 8, TILE))

    def widen(g):
        feats = []
        for value in (cols[g, 0], cols[g, 1], cols[g, 2], by_type(cols[g, 3], radius)):
            feats.extend(pieces(value))

        def put_block(d, k, value):
            wide[g * 8 + k, :, d] = value

        lanes_of(turn(feats), put_block)

    for k, zz in enumerate(far):
        origin = zz * 4 + x
        row_wait(core, origin)
        for j, xx in enumerate(side):
            send_row(origin, r, device(z, xx), 7 + 4 * k + j)
        send_row(origin, r, partner, 10 + 4 * k)

    def relay(k, slot):
        for j, xx in enumerate(side):
            origin = [z, *far][k] * 4 + xx
            row_wait(core, origin)
            send_row(origin, r, partner, slot + j)

    widen(r)
    col_wait(twin)
    for k, near in enumerate(yy):
        send_col(twin, zh * 4 + near, 4 + k)
    relay(0, 19)

    def near_cols(k, carry):
        origin = zh * 4 + lax.rem(y + k, 4)
        col_wait(origin)
        widen(origin)
        return carry

    lax.fori_loop(1, 4, near_cols, 0)
    for k in range(1, 4):
        relay(k, 19 + 3 * k)
    widen(twin)

    def far_cols(k, carry):
        origin = (1 - zh) * 4 + lax.rem(y + k, 4)
        col_wait(origin)
        widen(origin)
        return carry

    lax.fori_loop(1, 4, far_cols, 0)
    for p in range(CHIPS):
        row_wait(other, p)
    for par in range(2):
        for p in range(CHIPS):
            row_radius[par, p] = by_type(rows[par, p, 3], radius)

    def tile_of(s):
        a = tiles_ref[0, s]
        b = tiles_ref[1, s]
        return (a >> 3) & 1, a >> 4, a & 7, b

    def same_block(s):
        a = tiles_ref[0, s]
        b = tiles_ref[1, s]
        same = ((b >> 3) == r) & ((a >> 3) == c) & ((a & 7) == (b & 7))
        return jnp.where(same, F32(1), F32(0))

    def near_rows(s):
        sp, sq, sb, b = tile_of(s)
        near = [rows[sp, sq, d, pl.ds(sb, 1), :] for d in range(3)]
        return near, row_radius[sp, sq, pl.ds(sb, 1), :], b

    def over_tiles(fill, use, begin, end):
        fill(begin, buf_a)

        def body(t, carry):
            s = begin + 2 * t
            fill(s + 1, buf_b)
            use(s, buf_a)
            fill(jnp.minimum(s + 2, SLOTS - 1), buf_a)
            use(s + 1, buf_b)
            return carry

        lax.fori_loop(0, (end - begin) // 2, body, 0)

    def put(d, s, value):
        parts[d, pl.ds(s, 1), :] = jnp.sum(value, axis=0, keepdims=True)

    def first(s):
        near, near_r, b = near_rows(s)
        total = jnp.where(sub == 0, -same_block(s), F32(0))
        for k in range(16):
            dist = F32(0)
            for d in range(3):
                offset = near[d] - wide[b, k, d]
                dist = dist + offset * offset
            rho = near_r + wide[b, k, 3]
            ratio = dist / (rho * rho)
            total = total + jnp.exp2((ratio * ratio) * (ratio * F32(-LOG2E)))
        put(0, s, total)

    def by_eights(use):
        def body(t, carry):
            for k in range(8):
                use(8 * t + k)
            return carry

        lax.fori_loop(0, SLOTS // 8, body, 0)

    by_eights(first)

    def scatter(value):
        high = value.astype(BF16)
        low = (value - high.astype(F32)).astype(BF16)
        return high, low

    def spots(value):
        return value.reshape(2, CHIPS, 8, TILE)

    both = jnp.concatenate(scatter(parts[0]), axis=1)
    both = jnp.dot(onehot[...], both, preferred_element_type=F32)
    coord_part[...] = spots(both[:, :TILE] + both[:, TILE:])
    peers = [(par, p) for p in chips for par in (core, other)] + [(other, q)]
    for k, (par, p) in enumerate(peers):
        go(coord_part.at[par, p], coord_rx.at[core, q], c_send.at[k], c_recv.at[core, q], r, p * 2 + par)

    for g in range(8):
        feats = []
        for t in range(5):
            table = [depth_ref[t, u] * (valence[t] + valence[u]) for u in range(5)]
            feats.extend(pieces(by_type(cols[g, 3], table)))
        col_w[g] = turn(feats)

    def pair_terms(s, buf):
        sp, sq, sb, b = tile_of(s)
        kinds = jnp.broadcast_to(rows[sp, sq, 3, pl.ds(sb, 1), :], (8, TILE))
        kinds = jnp.where(sub == (b & 7), kinds, F32(-1))
        right = []
        for t in range(5):
            right.extend([jnp.where(kinds == F32(t), F32(1), F32(0))] * 3)
        right = jnp.concatenate(right + [blank], axis=0).astype(BF16)
        buf[...] = jnp.dot(col_w[b >> 3], right, preferred_element_type=F32)

    def prepare(s, buf):
        near, near_r, b = near_rows(s)
        same = same_block(s)
        for k in range(16):
            dx, dy, dz = (near[d] - wide[b, k, d] for d in range(3))
            rho = near_r + wide[b, k, 3]
            inverse = F32(1) / (rho * rho)
            ratio = (dx * dx + dy * dy + dz * dz) * inverse
            square = ratio * ratio
            numer = buf[8 * k : 8 * k + 8, :] * jnp.exp2(square * (ratio * F32(-LOG2E)))
            numer = jnp.where(lane_at == sub + 8 * k, numer * (F32(1) - same), numer)
            pull = numer * (square * inverse)
            store[s, k, 0] = pull * dx
            store[s, k, 1] = pull * dy
            store[s, k, 2] = pull * dz
            store[s, k, 3] = numer

    over_tiles(pair_terms, prepare, 0, EARLY)

    own = coord_part[core, q]
    for par, p in peers:
        block = coord_rx.at[par, p]
        copy(block, block, c_send.at[0], c_recv.at[par, p], r, p * 2 + par).wait_recv()
        own = own + coord_rx[par, p]
    own = own + by_type(rows[core, q, 3], valence)
    row_u[core, q] = own
    col_u[r] = own
    for k, p in enumerate(rows_of):
        go(col_u.at[r], col_u.at[r], v_send.at[k], v_recv.at[r], p, c)
    for k, p in enumerate(chips):
        go(row_u.at[core, q], row_u.at[core, q], u_send.at[k], u_recv.at[q], r, p * 2 + core)

    over_tiles(pair_terms, prepare, EARLY, SLOTS)

    for p in chips:
        block = row_u.at[core, p]
        copy(block, block, u_send.at[0], u_recv.at[p], r, p * 2 + core).wait_recv()
    go(row_u.at[core], row_u.at[core], pair_send.at[1], pair_recv.at[1], r, partner)
    for side_of in (zh, 1 - zh):
        for k in range(4):
            p = side_of * 4 + lax.rem(y + k, 4)
            if side_of is zh and k == 0:
                continue
            copy(col_u.at[p], col_u.at[p], v_send.at[0], v_recv.at[p], p, c).wait_recv()
        feats = []
        for k in range(4):
            feats.extend(pieces(col_u[4 * side_of + k]))

        def put_u(d, k, value, side_of=side_of):
            wide_u[side_of * 32 + d * 8 + k] = value

        lanes_of(turn(feats), put_u)
    copy(row_u.at[other], row_u.at[other], pair_send.at[1], pair_recv.at[1], r, partner).wait_recv()

    def second(s):
        sp, sq, sb, b = tile_of(s)
        near = row_u[sp, sq, pl.ds(sb, 1), :]
        total = [F32(0)] * 4
        for k in range(16):
            scale = F32(1) / (near + wide_u[b, k])
            for d in range(4):
                total[d] = total[d] + store[s, k, d] * scale
        for d in range(4):
            put(d, s, total[d])

    by_eights(second)

    sums = [scatter(jnp.concatenate([parts[d], parts[d + 1]], axis=1)) for d in (0, 2)]

    def gathered(par, ref):
        chosen = onehot[pl.ds(pl.multiple_of(par * TILE, TILE), TILE), :]
        for d, (high, low) in zip((0, 2), sums):
            both = jnp.dot(chosen, high, preferred_element_type=F32)
            both = both + jnp.dot(chosen, low, preferred_element_type=F32)
            ref[:, d] = both[:, :TILE].reshape(CHIPS, 8, TILE)
            ref[:, d + 1] = both[:, TILE:].reshape(CHIPS, 8, TILE)

    gathered(other, force_out)
    go(force_out, force_in, pair_send.at[2], pair_recv.at[2], r, partner)
    gathered(core, force_sum)
    copy(force_out, force_in, pair_send.at[2], pair_recv.at[2], r, partner).wait_recv()
    force_sum[...] = force_sum[...] + force_in[...]
    for k, p in enumerate(chips):
        go(force_sum.at[p], force_rx.at[q], f_send.at[k], f_recv.at[q], r, p * 2 + core)
    own = force_sum[q]
    for p in chips:
        copy(force_sum.at[0], force_rx.at[p], f_send.at[0], f_recv.at[p], r, p * 2 + core).wait_recv()
        own = own + force_rx[p]
    for k in range(8):
        out_ref[:, k * TILE : (k + 1) * TILE] = own[:, k, :]
    for descriptor in started:
        descriptor.wait_send()


def local(positions, types, radius_type, valence_type, bond_depth, pair_tiles, tile_count):
    vmem = pl.BlockSpec(memory_space=pltpu.VMEM)
    smem = pltpu.SMEM
    dma = pltpu.SemaphoreType.DMA
    sums = pl.pallas_call(
        kernel,
        out_shape=jax.ShapeDtypeStruct((4, positions.shape[1]), F32),
        in_specs=[pl.BlockSpec(memory_space=pltpu.HBM)] * 7,
        out_specs=vmem,
        scratch_shapes=[
            pltpu.VMEM(positions.shape, F32),
            pltpu.VMEM((8, TILE), jnp.int32),
            smem(radius_type.shape, F32),
            smem(valence_type.shape, F32),
            smem(bond_depth.shape, F32),
            smem((2, SLOTS), jnp.int32),
            smem((1, 1), jnp.int32),
            dma((7,)),
            pltpu.VMEM((2, CHIPS, 4, 8, TILE), F32),
            pltpu.VMEM((8, 4, 8, TILE), F32),
            pltpu.VMEM((2, CHIPS, 8, TILE), F32),
            pltpu.VMEM((2, CHIPS, 8, TILE), F32),
            pltpu.VMEM((8, 8, TILE), F32),
            pltpu.VMEM((16, TILE, 2 * TILE), BF16),
            pltpu.VMEM((64, 16, 4, 8, TILE), F32),
            pltpu.VMEM((64, 16, 8, TILE), F32),
            pltpu.VMEM((8, TILE, TILE), BF16),
            pltpu.VMEM((TILE, TILE), F32),
            pltpu.VMEM((TILE, TILE), F32),
            pltpu.VMEM((256, TILE), BF16),
            pltpu.VMEM((4, TILE, TILE), F32),
            pltpu.VMEM((SLOTS, 16, 4, 8, TILE), F32),
            pltpu.VMEM((2, CHIPS, 8, TILE), F32),
            pltpu.VMEM((2, CHIPS, 8, TILE), F32),
            pltpu.VMEM((CHIPS, 4, 8, TILE), F32),
            pltpu.VMEM((CHIPS, 4, 8, TILE), F32),
            pltpu.VMEM((CHIPS, 4, 8, TILE), F32),
            pltpu.VMEM((CHIPS, 4, 8, TILE), F32),
            dma((31,)), dma((2, CHIPS)), dma((7,)), dma((8,)), dma((3,)), dma((3,)),
            dma((31,)), dma((2, CHIPS)), dma((15,)), dma((CHIPS,)), dma((7,)), dma((8,)),
            dma((15,)), dma((CHIPS,)),
        ],
        compiler_params=pltpu.CompilerParams(
            collective_id=0, has_side_effects=True, vmem_limit_bytes=VMEM
        ),
    )(
        positions,
        types.reshape(8, TILE),
        radius_type,
        valence_type,
        bond_depth,
        pair_tiles.reshape(SLOTS, 2).T,
        tile_count,
    )
    component = lax.broadcasted_iota(jnp.int32, sums.shape, 0)
    return jnp.where(component < 3, F32(-6), F32(-1)) * sums


def solution(mesh):
    in_specs = (
        P(None, ("row", "col")),
        P(("row", "col")),
        P(),
        P(),
        P(),
        P("row", "col", None, None),
        P("row", "col"),
    )
    out_specs = P(None, ("row", "col"))
    return jax.shard_map(local, mesh=mesh, in_specs=in_specs, out_specs=out_specs, check_vma=False)
```

```python
import functools

import jax
import jax.numpy as jnp
from jax import lax
from jax.experimental import pallas as pl
from jax.experimental.pallas import tpu as pltpu
from jax.sharding import PartitionSpec as P

TILE = 128
SLOTS = 96
EARLY = 36
CHIPS = 16
VMEM = 56 * 1024 * 1024
MESH = pl.DeviceIdType.MESH
F32 = jnp.float32
BF16 = jnp.bfloat16
LOG2E = 1.4426950408889634


def pieces(value):
    high = value.astype(BF16).astype(F32)
    rest = value - high
    middle = rest.astype(BF16).astype(F32)
    return high, middle, rest - middle


def by_type(types, table):
    value = jnp.full(types.shape, table[0], F32)
    for t in range(1, len(table)):
        value = jnp.where(types == F32(t), table[t], value)
    return value


def kernel(
    pos_in, types_in, radius_in, valence_in, depth_in, tiles_in, count_in, out_ref,
    pos_ref, types_ref, radius_ref, valence_ref, depth_ref, tiles_ref, count_ref, load_sem,
    rows, cols, row_radius, row_u, col_u, pick_ref, wide, wide_u, col_w, buf_a, buf_b, onehot, parts, store,
    coord_part, coord_rx, force_out, force_in, force_sum, force_rx,
    row_send, row_recv, col_send, col_recv, pair_send, pair_recv,
    c_send, c_recv, u_send, u_recv, v_send, v_recv, f_send, f_recv,
):
    r = lax.axis_index("row")
    c = lax.axis_index("col")
    core = lax.rem(c, 2)
    q = c // 2
    z, x = q // 4, lax.rem(q, 4)
    zh, y = r // 4, lax.rem(r, 4)
    other = 1 - core

    def copy(src, dst, send, recv, row, col):
        return pltpu.make_async_remote_copy(
            src_ref=src, dst_ref=dst, send_sem=send, recv_sem=recv,
            device_id=(row, col), device_id_type=MESH,
        )

    chips = [lax.rem(q + k, CHIPS) for k in range(1, CHIPS)]
    rows_of = [lax.rem(r + k, 8) for k in range(1, 8)]

    def device(zz, xx):
        return (zz * 4 + xx) * 2 + core

    half = z // 2
    far = [z + 1 - 2 * lax.rem(z, 2), 2 - half, 3 * (1 - half)]
    side = [lax.rem(x + k, 4) for k in (2, 1, 3)]
    yy = [lax.rem(y + k, 4) for k in range(1, 4)]
    partner = q * 2 + other
    twin = (1 - zh) * 4 + y
    greeted = [(twin, c)]
    greeted += [(r, device(zz, x)) for zz in far]
    greeted += [(r, device(z, xx)) for xx in side]
    greeted += [(zh * 4 + near, c) for near in yy]
    greeted += [(r, partner)]
    barrier = pltpu.get_barrier_semaphore()
    inputs = (pos_in, types_in, radius_in, valence_in, depth_in, tiles_in, count_in)
    locals_ = (pos_ref, types_ref, radius_ref, valence_ref, depth_ref, tiles_ref, count_ref)
    loads = [pltpu.make_async_copy(a, b, load_sem.at[k]) for k, (a, b) in enumerate(zip(inputs, locals_))]
    for load in loads:
        load.start()

    for row, col in greeted:
        pl.semaphore_signal(barrier, inc=1, device_id=(row, col), device_id_type=MESH)

    sub = lax.broadcasted_iota(jnp.int32, (8, TILE), 0)
    blank = jnp.zeros((8, TILE), F32)
    for k in range(8):
        mark = jnp.where(sub == k, F32(1), F32(0))
        for d in range(4):
            column = [mark if 3 * d <= f < 3 * d + 3 else blank for f in range(16)]
            m = d * 8 + k
            at = slice(m % 2 * TILE, m % 2 * TILE + TILE)
            pick_ref[m // 2, :, at] = jnp.concatenate(column, axis=0).astype(BF16)

    for load in loads:
        load.wait()
    own_types = types_ref[...].astype(F32)
    for k in range(8):
        piece = pos_ref[:, k * TILE : (k + 1) * TILE]
        for d in range(3):
            rows[core, q, d, k : k + 1, :] = piece[d : d + 1]
            cols[r, d, k : k + 1, :] = piece[d : d + 1]
    rows[core, q, 3] = own_types
    cols[r, 3] = own_types

    pl.semaphore_wait(barrier, len(greeted))

    started = []

    def go(*args):
        descriptor = copy(*args)
        descriptor.start()
        started.append(descriptor)

    def send_row(origin, row, col, slot):
        block = rows.at[core, origin]
        go(block, block, row_send.at[slot], row_recv.at[core, origin], row, col)

    def send_col(origin, row, slot):
        block = cols.at[origin]
        go(block, block, col_send.at[slot], col_recv.at[origin], row, c)

    send_col(r, twin, 0)
    for k, zz in enumerate(far[::-1]):
        send_row(q, r, device(zz, x), k)
    for k, xx in enumerate(side):
        send_row(q, r, device(z, xx), 3 + k)
    for k, near in enumerate(yy):
        send_col(r, zh * 4 + near, 1 + k)
    send_row(q, r, partner, 6)

    def row_wait(par, origin):
        block = rows.at[par, origin]
        copy(block, block, row_send.at[0], row_recv.at[par, origin], r, partner).wait_recv()

    def col_wait(origin):
        block = cols.at[origin]
        copy(block, block, col_send.at[0], col_recv.at[origin], twin, c).wait_recv()

    live = count_ref[0, 0]
    lane_at = lax.broadcasted_iota(jnp.int32, (8, TILE), 1)

    def place_of(at, held):
        a = tiles_ref[0, at]
        place = ((a >> 3) & 1) * 128 + (a >> 4) * 8 + (a & 7)
        return jnp.where((lane_at == at) & (at < live), place, held)

    held = lax.fori_loop(0, SLOTS, place_of, jnp.full((8, TILE), -1, jnp.int32))
    match = lax.broadcasted_iota(jnp.int32, (256, TILE), 0) == held[0:1]
    onehot[...] = jnp.where(match, F32(1), F32(0)).astype(BF16)
    for d in range(4):
        parts[d, SLOTS:TILE, :] = jnp.zeros((TILE - SLOTS, TILE), F32)

    radius = [radius_ref[t] * F32(0.5) for t in range(5)]
    valence = [valence_ref[t] for t in range(5)]

    def turn(feats):
        feats = feats + [blank] * (16 - len(feats))
        return jnp.concatenate(feats, axis=0).T.astype(BF16)

    def lanes_of(left, put_block):
        for m in range(16):
            pair = jnp.dot(left, pick_ref[m], preferred_element_type=F32)
            for h in range(2):
                put_block((2 * m + h) // 8, (2 * m + h) % 8, pair[:, h * TILE : (h + 1) * TILE].reshape(16, 8, TILE))

    def widen(g):
        feats = []
        for value in (cols[g, 0], cols[g, 1], cols[g, 2], by_type(cols[g, 3], radius)):
            feats.extend(pieces(value))

        def put_block(d, k, value):
            wide[g * 8 + k, :, d] = value

        lanes_of(turn(feats), put_block)

    for k, zz in enumerate(far):
        origin = zz * 4 + x
        row_wait(core, origin)
        for j, xx in enumerate(side):
            send_row(origin, r, device(z, xx), 7 + 4 * k + j)
        send_row(origin, r, partner, 10 + 4 * k)

    def relay(k, slot):
        for j, xx in enumerate(side):
            origin = [z, *far][k] * 4 + xx
            row_wait(core, origin)
            send_row(origin, r, partner, slot + j)

    widen(r)
    col_wait(twin)
    for k, near in enumerate(yy):
        send_col(twin, zh * 4 + near, 4 + k)
    relay(0, 19)

    def near_cols(k, carry):
        origin = zh * 4 + lax.rem(y + k, 4)
        col_wait(origin)
        widen(origin)
        return carry

    lax.fori_loop(1, 4, near_cols, 0)
    for k in range(1, 4):
        relay(k, 19 + 3 * k)
    widen(twin)

    def far_cols(k, carry):
        origin = (1 - zh) * 4 + lax.rem(y + k, 4)
        col_wait(origin)
        widen(origin)
        return carry

    lax.fori_loop(1, 4, far_cols, 0)
    for p in range(CHIPS):
        row_wait(other, p)
    for par in range(2):
        for p in range(CHIPS):
            row_radius[par, p] = by_type(rows[par, p, 3], radius)

    def tile_of(s):
        a = tiles_ref[0, s]
        b = tiles_ref[1, s]
        return (a >> 3) & 1, a >> 4, a & 7, b

    def same_block(s):
        a = tiles_ref[0, s]
        b = tiles_ref[1, s]
        same = ((b >> 3) == r) & ((a >> 3) == c) & ((a & 7) == (b & 7))
        return jnp.where(same, F32(1), F32(0))

    def near_rows(s):
        sp, sq, sb, b = tile_of(s)
        near = [rows[sp, sq, d, pl.ds(sb, 1), :] for d in range(3)]
        return near, row_radius[sp, sq, pl.ds(sb, 1), :], b

    def over_tiles(fill, use, begin, end):
        fill(begin, buf_a)

        def body(t, carry):
            s = begin + 2 * t
            fill(s + 1, buf_b)
            use(s, buf_a)
            fill(jnp.minimum(s + 2, SLOTS - 1), buf_a)
            use(s + 1, buf_b)
            return carry

        lax.fori_loop(0, (end - begin) // 2, body, 0)

    def put(d, s, value):
        parts[d, pl.ds(s, 1), :] = jnp.sum(value, axis=0, keepdims=True)

    def first(s):
        near, near_r, b = near_rows(s)
        total = jnp.where(sub == 0, -same_block(s), F32(0))
        for k in range(16):
            dist = F32(0)
            for d in range(3):
                offset = near[d] - wide[b, k, d]
                dist = dist + offset * offset
            rho = near_r + wide[b, k, 3]
            ratio = dist / (rho * rho)
            total = total + jnp.exp2((ratio * ratio) * (ratio * F32(-LOG2E)))
        put(0, s, total)

    def by_eights(use):
        def body(t, carry):
            for k in range(8):
                use(8 * t + k)
            return carry

        lax.fori_loop(0, SLOTS // 8, body, 0)

    by_eights(first)

    def scatter(value):
        high = value.astype(BF16)
        low = (value - high.astype(F32)).astype(BF16)
        return high, low

    def spots(value):
        return value.reshape(2, CHIPS, 8, TILE)

    both = jnp.concatenate(scatter(parts[0]), axis=1)
    both = jnp.dot(onehot[...], both, preferred_element_type=F32)
    coord_part[...] = spots(both[:, :TILE] + both[:, TILE:])
    peers = [(par, p) for p in chips for par in (core, other)] + [(other, q)]
    for k, (par, p) in enumerate(peers):
        go(coord_part.at[par, p], coord_rx.at[core, q], c_send.at[k], c_recv.at[core, q], r, p * 2 + par)

    for g in range(8):
        feats = []
        for t in range(5):
            table = [depth_ref[t, u] * (valence[t] + valence[u]) for u in range(5)]
            feats.extend(pieces(by_type(cols[g, 3], table)))
        col_w[g] = turn(feats)

    def pair_terms(s, buf):
        sp, sq, sb, b = tile_of(s)
        kinds = jnp.broadcast_to(rows[sp, sq, 3, pl.ds(sb, 1), :], (8, TILE))
        kinds = jnp.where(sub == (b & 7), kinds, F32(-1))
        right = []
        for t in range(5):
            right.extend([jnp.where(kinds == F32(t), F32(1), F32(0))] * 3)
        right = jnp.concatenate(right + [blank], axis=0).astype(BF16)
        buf[...] = jnp.dot(col_w[b >> 3], right, preferred_element_type=F32)

    def prepare(s, buf):
        near, near_r, b = near_rows(s)
        same = same_block(s)
        for k in range(16):
            dx, dy, dz = (near[d] - wide[b, k, d] for d in range(3))
            rho = near_r + wide[b, k, 3]
            inverse = F32(1) / (rho * rho)
            ratio = (dx * dx + dy * dy + dz * dz) * inverse
            square = ratio * ratio
            numer = buf[8 * k : 8 * k + 8, :] * jnp.exp2(square * (ratio * F32(-LOG2E)))
            numer = jnp.where(lane_at == sub + 8 * k, numer * (F32(1) - same), numer)
            pull = numer * (square * inverse)
            store[s, k, 0] = pull * dx
            store[s, k, 1] = pull * dy
            store[s, k, 2] = pull * dz
            store[s, k, 3] = numer

    over_tiles(pair_terms, prepare, 0, EARLY)

    own = coord_part[core, q]
    for par, p in peers:
        block = coord_rx.at[par, p]
        copy(block, block, c_send.at[0], c_recv.at[par, p], r, p * 2 + par).wait_recv()
        own = own + coord_rx[par, p]
    own = own + by_type(rows[core, q, 3], valence)
    row_u[core, q] = own
    col_u[r] = own
    for k, p in enumerate(rows_of):
        go(col_u.at[r], col_u.at[r], v_send.at[k], v_recv.at[r], p, c)
    for k, p in enumerate(chips):
        go(row_u.at[core, q], row_u.at[core, q], u_send.at[k], u_recv.at[q], r, p * 2 + core)

    over_tiles(pair_terms, prepare, EARLY, SLOTS)

    for p in chips:
        block = row_u.at[core, p]
        copy(block, block, u_send.at[0], u_recv.at[p], r, p * 2 + core).wait_recv()
    go(row_u.at[core], row_u.at[core], pair_send.at[1], pair_recv.at[1], r, partner)
    for side_of in (zh, 1 - zh):
        for k in range(4):
            p = side_of * 4 + lax.rem(y + k, 4)
            if side_of is zh and k == 0:
                continue
            copy(col_u.at[p], col_u.at[p], v_send.at[0], v_recv.at[p], p, c).wait_recv()
        feats = []
        for k in range(4):
            feats.extend(pieces(col_u[4 * side_of + k]))

        def put_u(d, k, value, side_of=side_of):
            wide_u[side_of * 32 + d * 8 + k] = value

        lanes_of(turn(feats), put_u)
    copy(row_u.at[other], row_u.at[other], pair_send.at[1], pair_recv.at[1], r, partner).wait_recv()

    def second(s):
        sp, sq, sb, b = tile_of(s)
        near = row_u[sp, sq, pl.ds(sb, 1), :]
        total = [F32(0)] * 4
        for k in range(16):
            scale = F32(1) / (near + wide_u[b, k])
            for d in range(4):
                total[d] = total[d] + store[s, k, d] * scale
        for d in range(4):
            put(d, s, total[d])

    by_eights(second)

    sums = [scatter(jnp.concatenate([parts[d], parts[d + 1]], axis=1)) for d in (0, 2)]

    def gathered(par, ref):
        chosen = onehot[pl.ds(pl.multiple_of(par * TILE, TILE), TILE), :]
        for d, (high, low) in zip((0, 2), sums):
            both = jnp.dot(chosen, high, preferred_element_type=F32)
            both = both + jnp.dot(chosen, low, preferred_element_type=F32)
            ref[:, d] = both[:, :TILE].reshape(CHIPS, 8, TILE)
            ref[:, d + 1] = both[:, TILE:].reshape(CHIPS, 8, TILE)

    gathered(other, force_out)
    go(force_out, force_in, pair_send.at[2], pair_recv.at[2], r, partner)
    gathered(core, force_sum)
    copy(force_out, force_in, pair_send.at[2], pair_recv.at[2], r, partner).wait_recv()
    force_sum[...] = force_sum[...] + force_in[...]
    for k, p in enumerate(chips):
        go(force_sum.at[p], force_rx.at[q], f_send.at[k], f_recv.at[q], r, p * 2 + core)
    own = force_sum[q]
    for p in chips:
        copy(force_sum.at[0], force_rx.at[p], f_send.at[0], f_recv.at[p], r, p * 2 + core).wait_recv()
        own = own + force_rx[p]
    for k in range(8):
        out_ref[:, k * TILE : (k + 1) * TILE] = own[:, k, :]
    for descriptor in started:
        descriptor.wait_send()


def local(positions, types, radius_type, valence_type, bond_depth, pair_tiles, tile_count):
    vmem = pl.BlockSpec(memory_space=pltpu.VMEM)
    smem = pltpu.SMEM
    dma = pltpu.SemaphoreType.DMA
    sums = pl.pallas_call(
        kernel,
        out_shape=jax.ShapeDtypeStruct((4, positions.shape[1]), F32),
        in_specs=[pl.BlockSpec(memory_space=pltpu.HBM)] * 7,
        out_specs=vmem,
        scratch_shapes=[
            pltpu.VMEM(positions.shape, F32),
            pltpu.VMEM((8, TILE), jnp.int32),
            smem(radius_type.shape, F32),
            smem(valence_type.shape, F32),
            smem(bond_depth.shape, F32),
            smem((2, SLOTS), jnp.int32),
            smem((1, 1), jnp.int32),
            dma((7,)),
            pltpu.VMEM((2, CHIPS, 4, 8, TILE), F32),
            pltpu.VMEM((8, 4, 8, TILE), F32),
            pltpu.VMEM((2, CHIPS, 8, TILE), F32),
            pltpu.VMEM((2, CHIPS, 8, TILE), F32),
            pltpu.VMEM((8, 8, TILE), F32),
            pltpu.VMEM((16, TILE, 2 * TILE), BF16),
            pltpu.VMEM((64, 16, 4, 8, TILE), F32),
            pltpu.VMEM((64, 16, 8, TILE), F32),
            pltpu.VMEM((8, TILE, TILE), BF16),
            pltpu.VMEM((TILE, TILE), F32),
            pltpu.VMEM((TILE, TILE), F32),
            pltpu.VMEM((256, TILE), BF16),
            pltpu.VMEM((4, TILE, TILE), F32),
            pltpu.VMEM((SLOTS, 16, 4, 8, TILE), F32),
            pltpu.VMEM((2, CHIPS, 8, TILE), F32),
            pltpu.VMEM((2, CHIPS, 8, TILE), F32),
            pltpu.VMEM((CHIPS, 4, 8, TILE), F32),
            pltpu.VMEM((CHIPS, 4, 8, TILE), F32),
            pltpu.VMEM((CHIPS, 4, 8, TILE), F32),
            pltpu.VMEM((CHIPS, 4, 8, TILE), F32),
            dma((31,)), dma((2, CHIPS)), dma((7,)), dma((8,)), dma((3,)), dma((3,)),
            dma((31,)), dma((2, CHIPS)), dma((15,)), dma((CHIPS,)), dma((7,)), dma((8,)),
            dma((15,)), dma((CHIPS,)),
        ],
        compiler_params=pltpu.CompilerParams(
            collective_id=0, has_side_effects=True, vmem_limit_bytes=VMEM
        ),
    )(
        positions,
        types.reshape(8, TILE),
        radius_type,
        valence_type,
        bond_depth,
        pair_tiles.reshape(SLOTS, 2).T,
        tile_count,
    )
    component = lax.broadcasted_iota(jnp.int32, sums.shape, 0)
    return jnp.where(component < 3, F32(-6), F32(-1)) * sums


def solution(mesh):
    in_specs = (
        P(None, ("row", "col")),
        P(("row", "col")),
        P(),
        P(),
        P(),
        P("row", "col", None, None),
        P("row", "col"),
    )
    out_specs = P(None, ("row", "col"))
    return jax.shard_map(local, mesh=mesh, in_specs=in_specs, out_specs=out_specs, check_vma=False)
```
